256 devices in a mesh: grp: 32 (over z_hi, y, core), tp: 8 (over z_lo, x).
Axes of the slice: x: 4, y: 4, z: 8 (z_hi: 4, z_lo: 2; z = z_hi * 2 + z_lo), core: 2. Of those that a mesh axis runs over, the one named last changes fastest.
Arguments:
- tokens: bfloat16 [2048, 6144], P('grp', 'tp'), may hold values from -6 to 6
- norm_gain: float32 [6144], replicated, may hold values from 0.25 to 1.75
- router_weight: bfloat16 [6144, 8], replicated, may hold values from -0.078125 to 0.078125
- expert_ids: int32 [2048, 2], P('grp'), may hold values from 0 to 7, all different within a row; in each aligned block of 64 rows (0 to 63, 64 to 127, ...) at most 18 rows name the same one
- gate_proj: bfloat16 [6144, 65536], P(None, ('grp', 'tp')), may hold values from -0.078125 to 0.078125
- up_proj: bfloat16 [6144, 65536], P(None, ('grp', 'tp')), may hold values from -0.078125 to 0.078125
- down_proj: bfloat16 [65536, 6144], P(('grp', 'tp')), may hold values from -0.25 to 0.25
Outputs:
- mixed: bfloat16 [2048, 6144], P('grp', 'tp')
The draws below stay inside these ranges and needn't reach their ends.
Inputs may be any that keep to these rules, and one draw needn't show every extreme that they name: `expert_ids`: each row names two different experts; within the rows of one group (aligned blocks of 64 rows) no expert is named more than 18 times, and in some group one expert is named exactly 18 times.
All inputs are finite; a program needn't handle non-finite values.
Results may differ from the reference program's by a relative error of at most 0.017.
Values may be sent and summed in bfloat16 or wider, within the bound.
No kernel may reach another device: no remote copies, remote signals or barrier semaphores. Data moves between devices by JAX's collectives and lax.ppermute only.
A program may use at most 128 MiB of HBM per device.

```python
import math
import jax
import jax.numpy as jnp
import numpy as np
from jax import lax

D = 6144
EXPERTS = 8
FF = 8192
TOK_GRP = 64
CAP = 18
TOKENS = 2048
N_GRP = 32
N_TP = 8


def with_spikes(values, own_key, source, target, blocks, factor):
    def block_of(axis_at):
        return (jnp.arange(values.shape[axis_at]) // (values.shape[axis_at] // blocks)).reshape((-1,) + (1,) * (values.ndim - 1 - axis_at))

    first = jax.random.permutation(own_key, blocks)[block_of(target)]
    far = (block_of(target) + blocks // 2) % blocks
    return jnp.where((block_of(source) == first) | (block_of(source) == far), factor * values, values)


def levels(stream_key, dims, shards, low, top_value):
    def one(axis_at, blocks):
        steps = jax.random.uniform(jax.random.fold_in(jax.random.fold_in(stream_key, 6), axis_at), (blocks,), jnp.float32, low / len(shards), top_value / len(shards))
        return jnp.repeat(jnp.exp(steps), dims[axis_at] // blocks).reshape((-1,) + (1,) * (len(dims) - axis_at - 1))

    factor_of = one(*shards[0])
    for cut in shards[1:]:
        factor_of = factor_of * one(*cut)
    return factor_of


def deal_out(own_key, own, number, rows, amount, top, limit, skew):
    order = jax.random.permutation(own_key, amount)
    crowded, ordinary = shares(amount, rows * top, limit, skew, True), shares(amount, rows * top, limit, skew, False)
    places = jnp.arange(amount)

    def named(sizes, turn):
        used = int((sizes > 0).sum())
        fixed = max(1, used // 4)
        moved = fixed + (places - fixed + turn * (used - fixed)) % max(1, amount - fixed)
        return jnp.zeros((amount,), jnp.int32).at[order[jnp.where(places < fixed, places, moved)]].set(jnp.asarray(sizes, jnp.int32))

    sizes = jnp.where(number % 4 == 0, named(crowded, number // 4), named(ordinary, number - number // 4 - 1))
    mixed = jax.random.permutation(jax.random.fold_in(own, 3), amount)
    giver, sink = mixed[0:amount // 2 * 2:2], mixed[1:amount // 2 * 2:2]
    margin = jnp.minimum(sizes[giver] - 1, limit - sizes[sink]) // 2
    margin = jnp.where((giver == order[0]) | (sink == order[0]) | (sizes[sink] == 0), 0, jnp.maximum(margin, 0))
    moved = jax.random.randint(jax.random.fold_in(own, 4), (amount // 2,), 0, 1 << 20) % (margin + 1)
    sizes = sizes.at[giver].add(-moved).at[sink].add(moved)
    labels = jnp.searchsorted(jnp.cumsum(sizes), jnp.arange(rows * top), side="right").astype(jnp.int32)
    table = labels.reshape(top, rows).T
    table = table[jax.random.permutation(jax.random.fold_in(own, 1), rows)]
    turn = jax.random.randint(jax.random.fold_in(own, 2), (rows, 1), 0, top)
    return jnp.take_along_axis(table, (jnp.arange(top)[None, :] + turn) % top, axis=1)


def shares(amount, total, most, slope, full):
    loads = [(1 << 20) // math.isqrt(standing ** slope) + 1 for standing in range(1, amount + 1)]
    largest = most if full else min(most, max(-(-total // amount), total * loads[0] // sum(loads)))
    least = 1 if total - largest >= amount - 1 else 0
    holding, surplus = [largest] + [least] * (amount - 1), total - largest - least * (amount - 1)
    while surplus > 0:
        candidates = [i for i in range(1, amount) if holding[i] < largest] or [i for i in range(1, amount) if holding[i] < most]
        whole, left = sum([loads[i] for i in candidates]), surplus
        for i in candidates:
            more = min(most - holding[i], max(1, left * loads[i] // whole), surplus)
            holding[i] = holding[i] + more
            surplus = surplus - more
    return np.array(holding)


def gaussian(key, shape, spread, bound, cuts=(), held_as=jnp.bfloat16):
    entries = jax.random.normal(key, shape, jnp.float32) * spread
    if len(cuts) > 0:
        entries = levels(key, shape, cuts, -0.22, 0.18) * entries
    return jnp.clip(entries, min=-bound, max=bound).astype(held_as)


def gaussian_with(rng, extent, width, most, split, heavy, held_as=jnp.bfloat16):
    drawn = width * jax.random.normal(rng, extent, jnp.float32)
    if split:
        drawn = drawn * levels(rng, extent, split, -0.22, 0.18)
    return jnp.clip(with_spikes(drawn, jax.random.fold_in(rng, 3), *heavy), -most, most).astype(held_as)


def setup_inputs(seed: int = 0) -> dict:
    streams_of = jax.random.split(jax.random.key(seed), 8)
    tokens = gaussian(streams_of[0], (TOKENS, D), 1.0, 6.0, ((0, 32), (1, 8)))
    norm_gain = jnp.clip(1.0 + 0.15 * jax.random.normal(streams_of[1], (D,), jnp.float32), 0.25, 1.75)
    router_weight = gaussian(streams_of[2], (D, EXPERTS), D ** -0.5, 0.078125)
    expert_ids_keys = jax.random.split(jax.random.fold_in(streams_of[3], 1), TOKENS // TOK_GRP)
    expert_ids_turns = jax.random.permutation(jax.random.fold_in(streams_of[3], 3), TOKENS // TOK_GRP)
    expert_ids = jax.vmap(lambda own, number: deal_out(jax.random.fold_in(streams_of[3], 2), own, number, TOK_GRP, EXPERTS, 2, CAP, 1))(expert_ids_keys, expert_ids_turns).reshape((TOKENS, 2))
    gate_proj = gaussian(streams_of[4], (D, EXPERTS * FF), D ** -0.5, 0.078125, ((1, 256),))
    up_proj = gaussian(streams_of[5], (D, EXPERTS * FF), D ** -0.5, 0.078125, ((1, 256),))
    down_proj = gaussian_with(streams_of[6], (EXPERTS * FF, D), FF ** -0.5, 0.25, ((0, 256),), (0, 1, 256, 6.0))
    return dict(tokens=tokens, norm_gain=norm_gain, router_weight=router_weight, expert_ids=expert_ids, gate_proj=gate_proj, up_proj=up_proj, down_proj=down_proj)


def reference(tokens, norm_gain, router_weight, expert_ids, gate_proj, up_proj, down_proj):
    epsilon = 1e-05
    values = tokens.astype(jnp.float32)
    mean_square = lax.optimization_barrier(jnp.mean(values * values, axis=-1, keepdims=True))
    normed = (values * lax.rsqrt(mean_square + epsilon) * norm_gain).astype(jnp.bfloat16)
    logits = jnp.dot(normed, router_weight, preferred_element_type=jnp.float32)
    chosen = jnp.take_along_axis(logits, expert_ids, axis=1)
    gate_first = 1.0 / (1.0 + jnp.exp(chosen[:, 1] - chosen[:, 0]))
    gate_second = 1.0 / (1.0 + jnp.exp(chosen[:, 0] - chosen[:, 1]))
    gates = jnp.stack([gate_first, gate_second], axis=1)
    owners = N_GRP // EXPERTS
    slice_width = FF // (owners * N_TP)
    group_ids = expert_ids.reshape(N_GRP, TOK_GRP, 2)
    group_gates = gates.reshape(N_GRP, TOK_GRP, 2)
    mixed = jnp.zeros((TOKENS, D), jnp.float32)
    for expert in range(EXPERTS):
        hits = (group_ids == expert).astype(jnp.int32)
        routed = lax.optimization_barrier(jnp.sum(hits, axis=-1))
        gate_table = lax.optimization_barrier(jnp.sum(group_gates * hits.astype(jnp.float32), axis=-1))
        order = jnp.argsort(1 - routed, axis=1, stable=True)[:, :CAP].astype(jnp.int32)
        valid = jnp.take_along_axis(routed, order, axis=1).astype(jnp.float32)
        token_index = (order + jnp.arange(N_GRP, dtype=jnp.int32)[:, None] * TOK_GRP).reshape(-1)
        row_weight = (jnp.take_along_axis(gate_table, order, axis=1) * valid).reshape(-1)
        row_block = normed[token_index]
        total = jnp.zeros((N_GRP * CAP, D), jnp.float32)
        for quarter in range(owners):
            quarter_sum = jnp.zeros((N_GRP * CAP, D), jnp.float32)
            for piece in range(N_TP):
                column = expert * FF + (quarter * N_TP + piece) * slice_width
                gate_act = jnp.dot(row_block, gate_proj[:, column:column + slice_width], preferred_element_type=jnp.float32)
                up_act = jnp.dot(row_block, up_proj[:, column:column + slice_width], preferred_element_type=jnp.float32)
                hidden = (jax.nn.silu(gate_act) * up_act).astype(jnp.bfloat16)
                partial_out = jnp.dot(hidden, down_proj[column:column + slice_width], preferred_element_type=jnp.float32).astype(jnp.bfloat16)
                quarter_sum = quarter_sum + lax.optimization_barrier(partial_out).astype(jnp.float32)
            total = total + lax.optimization_barrier(quarter_sum.astype(jnp.bfloat16)).astype(jnp.float32)
        mixed = mixed.at[token_index].add(total * row_weight[:, None])
    return mixed.astype(jnp.bfloat16)
```

```python
from functools import partial

import jax
import jax.numpy as jnp
from jax import lax
from jax.experimental import pallas as pl
from jax.experimental.pallas import tpu as pltpu
from jax.sharding import Mesh
from jax.sharding import PartitionSpec as P


AXES = ("zh", "y2", "y1", "c", "zl", "x")
SIZES = (4, 2, 2, 2, 2, 4)
GRP = ("zh", "y2", "y1", "c")
TP = ("zl", "x")
OWNER = ("y1", "c", "zl", "x")
CAP = 18
SLOT = 24
SENDERS = 8
ROWS = SENDERS * CAP
PADDED = SENDERS * SLOT
EPSILON = 1e-05
F32 = jnp.float32
BF16 = jnp.bfloat16


def place(y, z, x, step):
    if step == "x+":
        return y, z, (x + 1) % 4
    if step == "x-":
        return y, z, (x - 1) % 4
    if step == "y":
        return 1 - y, z, x
    return y, 1 - z, x


def owner_pairs(step_core0, step_core1):
    pairs = []
    for y in range(2):
        for core, step in enumerate((step_core0, step_core1)):
            for z in range(2):
                for x in range(4):
                    y_to, z_to, x_to = place(y, z, x, step)
                    source = ((y * 2 + core) * 2 + z) * 4 + x
                    target = ((y_to * 2 + core) * 2 + z_to) * 4 + x_to
                    pairs.append((source, target))
    return pairs


def hop(value, step_core0, step_core1):
    return lax.ppermute(value, OWNER, owner_pairs(step_core0, step_core1))


def send_pairs(k, back):
    pairs = []
    for z in range(4):
        for y in range(2):
            source, target = z * 2 + y, (z + (k >> 1)) % 4 * 2 + (y ^ (k & 1))
            pairs.append((target, source) if back else (source, target))
    return pairs


def to_owner(value, k):
    return value if k == 0 else lax.ppermute(value, ("zh", "y2"), send_pairs(k, False))


def to_home(value, k):
    return value if k == 0 else lax.ppermute(value, ("zh", "y2"), send_pairs(k, True))


def whole(count):
    return [pl.BlockSpec(memory_space=pltpu.VMEM)] * count


def slots_of(ids):
    rows = ids.shape[0]
    lane = lax.broadcasted_iota(jnp.int32, (rows, PADDED), 1)
    k = (lane * 171) >> 12
    inside = lane - k * SLOT
    zh, y2 = lax.axis_index("zh"), lax.axis_index("y2")
    expert = ((zh + (k >> 1)) & 3) * 2 + (y2 ^ (k & 1))
    first, second = ids[:, 0:1] == expert, ids[:, 1:2] == expert
    routed = jnp.where(first | second, 1.0, 0.0)
    earlier = lax.broadcasted_iota(jnp.int32, (rows, rows), 1) < lax.broadcasted_iota(
        jnp.int32, (rows, rows), 0
    )
    before = jnp.dot(
        jnp.where(earlier, 1.0, 0.0).astype(BF16), routed.astype(BF16), preferred_element_type=F32
    )
    here = before == inside.astype(F32)
    return first & here, second & here


def select_kernel(ids_ref, tokens_ref, *out_refs):
    first, second = slots_of(ids_ref[...])
    picks = jnp.where(first | second, 1.0, 0.0).astype(BF16)
    chosen = lax.dot_general(
        picks, tokens_ref[...], (((0,), (0,)), ((), ())), preferred_element_type=F32
    )
    for k, out in enumerate(out_refs):
        out[...] = chosen[k * SLOT : (k + 1) * SLOT].astype(BF16)


def select(ids, tokens):
    out = jax.ShapeDtypeStruct((SLOT, tokens.shape[1]), BF16)
    return pl.pallas_call(
        select_kernel,
        out_shape=[out] * SENDERS,
        in_specs=whole(2),
        out_specs=whole(SENDERS),
        compiler_params=pltpu.CompilerParams(vmem_limit_bytes=4 << 20),
        name="select",
    )(ids, tokens)


def packing(shape, row_axis):
    row = lax.broadcasted_iota(jnp.int32, shape, row_axis)
    slot = lax.broadcasted_iota(jnp.int32, shape, 1 - row_axis)
    k = (slot * 171) >> 12
    inside = slot - k * SLOT
    return jnp.where((k * CAP + inside == row) & (inside < CAP), 1.0, 0.0).astype(BF16)


def pack_kernel(*refs):
    *blocks, out_ref = refs
    rows = jnp.concatenate([b[...] for b in blocks], axis=0)
    out_ref[...] = jnp.dot(
        packing((ROWS, PADDED), 0), rows, preferred_element_type=F32
    ).astype(BF16)


def pack(blocks):
    return pl.pallas_call(
        pack_kernel,
        out_shape=jax.ShapeDtypeStruct((ROWS, blocks[0].shape[1]), BF16),
        in_specs=whole(SENDERS),
        out_specs=whole(1)[0],
        compiler_params=pltpu.CompilerParams(vmem_limit_bytes=4 << 20),
        name="pack",
    )(*blocks)


def unpack_kernel(*refs):
    terms, out_refs = refs[:3], refs[3:]
    total = (terms[0][...].astype(F32) + terms[1][...].astype(F32) + terms[2][...].astype(F32)).astype(
        BF16
    )
    slots = jnp.dot(packing((PADDED, ROWS), 1), total, preferred_element_type=F32)
    for k, out in enumerate(out_refs):
        out[...] = slots[k * SLOT : (k + 1) * SLOT].astype(BF16)


def unpack(*terms):
    out = jax.ShapeDtypeStruct((SLOT, terms[0].shape[1]), BF16)
    return pl.pallas_call(
        unpack_kernel,
        out_shape=[out] * SENDERS,
        in_specs=whole(3),
        out_specs=whole(SENDERS),
        compiler_params=pltpu.CompilerParams(vmem_limit_bytes=4 << 20),
        name="unpack",
    )(*terms)


def stats_kernel(tokens_ref, gain_ref, router_ref, out_ref):
    width = tokens_ref.shape[1]
    part = lax.axis_index("zl") * 4 + lax.axis_index("x")
    start = pl.multiple_of(part * width, width)
    values = tokens_ref[...].astype(F32)
    scaled = values * gain_ref[:, pl.ds(start, width)]
    router = router_ref[pl.ds(start, width), :]
    high = scaled.astype(BF16)
    low = (scaled - high.astype(F32)).astype(BF16)
    logits = jnp.dot(high, router, preferred_element_type=F32) + jnp.dot(
        low, router, preferred_element_type=F32
    )
    squares = jnp.sum(values * values, axis=1, keepdims=True)
    rows, experts = logits.shape
    out_ref[...] = jnp.concatenate(
        [logits, jnp.broadcast_to(squares, (rows, 128 - experts))], axis=1
    )


def stats(tokens, gain, router):
    return pl.pallas_call(
        stats_kernel,
        out_shape=jax.ShapeDtypeStruct((tokens.shape[0], 128), F32),
        in_specs=whole(3),
        out_specs=whole(1)[0],
        compiler_params=pltpu.CompilerParams(vmem_limit_bytes=8 << 20),
        name="stats",
    )(tokens, gain, router)


def combine_kernel(width_all, experts, ids_ref, sums_ref, *refs):
    *blocks, out_ref = refs
    ids = ids_ref[...]
    sums = sums_ref[...]
    scale = lax.rsqrt(sums[:, experts : experts + 1] / width_all + EPSILON)
    lane = lax.broadcasted_iota(jnp.int32, sums.shape, 1)
    logits = [
        jnp.sum(jnp.where(lane == ids[:, k : k + 1], sums, 0.0), axis=1, keepdims=True) * scale
        for k in (0, 1)
    ]
    gate_first = 1.0 / (1.0 + jnp.exp(logits[1] - logits[0]))
    gate_second = 1.0 / (1.0 + jnp.exp(logits[0] - logits[1]))
    first, second = slots_of(ids)
    weights = jnp.where(first, gate_first, 0.0) + jnp.where(second, gate_second, 0.0)
    high = weights.astype(BF16)
    low = (weights - high.astype(F32)).astype(BF16)
    rows = jnp.concatenate([b[...] for b in blocks], axis=0)
    out_ref[...] = (
        jnp.dot(high, rows, preferred_element_type=F32)
        + jnp.dot(low, rows, preferred_element_type=F32)
    ).astype(BF16)


def combine(width_all, experts, ids, sums, blocks):
    return pl.pallas_call(
        partial(combine_kernel, width_all, experts),
        out_shape=jax.ShapeDtypeStruct((ids.shape[0], blocks[0].shape[1]), BF16),
        in_specs=whole(2 + SENDERS),
        out_specs=whole(1)[0],
        compiler_params=pltpu.CompilerParams(vmem_limit_bytes=4 << 20),
        name="combine",
    )(ids, sums, *blocks)


def tile_place(m, a):
    core = lax.axis_index("c")
    square = jnp.where(core == 0, m, a)
    ring = jnp.where(core == 0, a, m)
    row_class = square & 1
    offset = jnp.where(ring == 1, 3, jnp.where(ring == 2, 1, jnp.where(ring == 3, 2, 0)))
    feature = (lax.axis_index("zl") ^ (square >> 1)) * 4 + ((lax.axis_index("x") + offset) & 3)
    return row_class, feature


def hidden_kernel(width_all, gain_ref, *refs):
    tiles, weights = refs[:16], refs[16:20]
    out_ref, x_ref, w_ref, squares_ref, sems = refs[20:]
    copies = [pltpu.make_async_copy(w, w_ref.at[n], sems.at[n]) for n, w in enumerate(weights)]
    for copy in copies:
        copy.start()
    rows, width = tiles[0].shape
    slices = w_ref.shape[2]
    squares_ref[...] = jnp.zeros_like(squares_ref)
    for index, tile in enumerate(tiles):
        row_class, feature = tile_place(index // 4, index % 4)
        row_at = pl.ds(pl.multiple_of(row_class * rows, rows), rows)
        column_at = pl.ds(pl.multiple_of(feature * width, width), width)
        values = tile[...].astype(F32)
        x_ref[row_at, column_at] = (values * gain_ref[:, column_at]).astype(BF16)
        square = values * values
        squares_ref[row_at, :] += sum(
            square[:, j * 128 : (j + 1) * 128] for j in range(width // 128)
        )
    scale = lax.rsqrt(jnp.sum(squares_ref[...], axis=1, keepdims=True) / width_all + EPSILON)
    for half in range(2):
        copies[2 * half].wait()
        gate = jnp.dot(x_ref[...], w_ref[2 * half], preferred_element_type=F32) * scale
        copies[2 * half + 1].wait()
        up = jnp.dot(x_ref[...], w_ref[2 * half + 1], preferred_element_type=F32) * scale
        out_ref[:, half * slices : (half + 1) * slices] = (
            gate * (1.0 / (1.0 + jnp.exp(-gate))) * up
        ).astype(BF16)


def hidden_of(gain, tiles, gates_ups):
    rows, width = tiles[0].shape
    width_all, slices = gates_ups[0].shape
    return pl.pallas_call(
        partial(hidden_kernel, width_all),
        out_shape=jax.ShapeDtypeStruct((2 * rows, 2 * slices), BF16),
        in_specs=whole(17) + [pl.BlockSpec(memory_space=pl.ANY)] * 4,
        out_specs=whole(1)[0],
        scratch_shapes=[
            pltpu.VMEM((2 * rows, width_all), BF16),
            pltpu.VMEM((4, width_all, slices), BF16),
            pltpu.VMEM((2 * rows, 128), F32),
            pltpu.SemaphoreType.DMA((4,)),
        ],
        compiler_params=pltpu.CompilerParams(vmem_limit_bytes=32 << 20),
        cost_estimate=pl.CostEstimate(
            flops=2 * 2 * rows * width_all * 4 * slices,
            bytes_accessed=4 * width_all * slices * 2,
            transcendentals=0,
        ),
        name="hidden",
    )(gain, *tiles, *gates_ups)


def down_kernel(wanted, hidden_ref, own_ref, other_ref, *refs):
    out_refs, (w_ref, sems) = refs[: len(wanted)], refs[len(wanted) :]
    slices = own_ref.shape[0]
    rows, width = out_refs[0].shape
    copies = []
    for n, (m, a) in enumerate(wanted):
        _, feature = tile_place(m, a)
        column_at = pl.ds(pl.multiple_of(feature * width, width), width)
        pair = [
            pltpu.make_async_copy(
                w.at[:, column_at], w_ref.at[n, pl.ds(h * slices, slices)], sems.at[n, h]
            )
            for h, w in enumerate((own_ref, other_ref))
        ]
        for copy in pair:
            copy.start()
        copies.append(pair)
    for n, (m, a) in enumerate(wanted):
        row_class, _ = tile_place(m, a)
        row_at = pl.ds(pl.multiple_of(row_class * rows, rows), rows)
        for copy in copies[n]:
            copy.wait()
        out_refs[n][...] = jnp.dot(
            hidden_ref[row_at, :], w_ref[n], preferred_element_type=F32
        ).astype(BF16)


def down_of(wanted, rows, width, hidden, own, other):
    out = jax.ShapeDtypeStruct((rows, width), BF16)
    slices = own.shape[0]
    return pl.pallas_call(
        partial(down_kernel, wanted),
        out_shape=[out] * len(wanted),
        in_specs=whole(1) + [pl.BlockSpec(memory_space=pl.ANY)] * 2,
        out_specs=whole(len(wanted)),
        scratch_shapes=[
            pltpu.VMEM((len(wanted), 2 * slices, width), BF16),
            pltpu.SemaphoreType.DMA((len(wanted), 2)),
        ],
        compiler_params=pltpu.CompilerParams(vmem_limit_bytes=24 << 20),
        cost_estimate=pl.CostEstimate(
            flops=2 * rows * width * 2 * slices * len(wanted),
            bytes_accessed=len(wanted) * 2 * slices * width * 2,
            transcendentals=0,
        ),
        name="down",
    )(hidden, own, other)


def added(*terms):
    return sum(t.astype(F32) for t in terms).astype(BF16)


def per_device(tokens, norm_gain, router_weight, expert_ids, gate_proj, up_proj, down_proj):
    width_all, experts = router_weight.shape
    width = tokens.shape[1]
    gain = norm_gain.reshape(1, width_all)

    blocks = select(expert_ids, tokens)
    arrived = [to_owner(block, k) for k, block in enumerate(blocks)]
    swap = [(0, 1), (1, 0)]
    gate_other = lax.ppermute(gate_proj, "c", swap)
    up_other = lax.ppermute(up_proj, "c", swap)
    down_other = lax.ppermute(down_proj, "c", swap)
    mine = pack(arrived)

    sums = stats(tokens, gain, router_weight)
    for distance in (1, 2, 4):
        sums = sums + lax.ppermute(sums, TP, [(i, i ^ distance) for i in range(8)])

    inner = [mine, hop(mine, "x+", "y"), hop(mine, "x-", "z")]
    inner.append(hop(inner[1], "x+", "z"))
    outer = [inner, [], [], [None] * 4]
    for a in range(4):
        outer[1].append(hop(inner[a], "y", "x+"))
        outer[2].append(hop(inner[a], "z", "x-"))
    for a in (0, 1):
        outer[3][a] = hop(outer[1][a], "z", "x+")
    for a in (2, 3):
        outer[3][a] = hop(outer[2][a], "y", "x-")
    tiles = [outer[m][a] for m in range(4) for a in range(4)]

    hidden = hidden_of(gain, tiles, (gate_proj, up_proj, gate_other, up_other))

    def partials(m):
        wanted = [(m, a) for a in range(4)]
        return down_of(wanted, ROWS, width, hidden, down_proj, down_other)

    far = partials(3)
    near = [None, list(partials(1)), list(partials(2))]
    own = partials(0)
    for a in (0, 1):
        near[1][a] = added(near[1][a], hop(far[a], "z", "x-"))
    for a in (2, 3):
        near[2][a] = added(near[2][a], hop(far[a], "y", "x+"))
    total = [
        added(own[a], hop(near[1][a], "y", "x-"), hop(near[2][a], "z", "x+")) for a in range(4)
    ]
    second = added(total[1], hop(total[3], "x-", "z"))
    results = unpack(total[0], hop(second, "x-", "y"), hop(total[2], "x+", "z"))
    returned = [to_home(block, k) for k, block in enumerate(results)]
    return combine(width_all, experts, expert_ids, sums, returned)


def solution(mesh):
    cut = Mesh(mesh.devices.reshape(SIZES), AXES)
    split = GRP + TP
    placed = (
        P(GRP, TP),
        P(),
        P(),
        P(GRP, None),
        P(None, split),
        P(None, split),
        P(split, None),
    )
    return jax.shard_map(
        per_device, mesh=cut, in_specs=placed, out_specs=P(GRP, TP), check_vma=False
    )
```

```python
from functools import partial

import jax
import jax.numpy as jnp
from jax import lax
from jax.experimental import pallas as pl
from jax.experimental.pallas import tpu as pltpu
from jax.sharding import Mesh
from jax.sharding import PartitionSpec as P


AXES = ("zh", "y2", "y1", "c", "zl", "x")
SIZES = (4, 2, 2, 2, 2, 4)
GRP = ("zh", "y2", "y1", "c")
TP = ("zl", "x")
OWNER = ("y1", "c", "zl", "x")
CAP = 18
FAR = 4
KEPT = FAR * CAP
ROWS = 2 * KEPT
EXTRA = 8
BLOCK = 40
EPSILON = 1e-05
F32 = jnp.float32
BF16 = jnp.bfloat16


def place(y, z, x, step):
    if step == "x+":
        return y, z, (x + 1) % 4
    if step == "x-":
        return y, z, (x - 1) % 4
    if step == "xx":
        return y, z, (x + 2) % 4
    if step == "y":
        return 1 - y, z, x
    if step == "z":
        return y, 1 - z, x
    return 1 - y, 1 - z, x


def owner_pairs(step_core0, step_core1):
    pairs = []
    for y in range(2):
        for core, step in enumerate((step_core0, step_core1)):
            for z in range(2):
                for x in range(4):
                    y_to, z_to, x_to = place(y, z, x, step)
                    source = ((y * 2 + core) * 2 + z) * 4 + x
                    target = ((y_to * 2 + core) * 2 + z_to) * 4 + x_to
                    pairs.append((source, target))
    return pairs


def hop(value, step_core0, step_core1):
    return lax.ppermute(value, OWNER, owner_pairs(step_core0, step_core1))


def along_z(value, distance):
    return lax.ppermute(value, "zh", [(i, (i + distance) % FAR) for i in range(FAR)])


def across_y(value):
    return lax.ppermute(value, ("y2", "y1"), [(i, 3 - i) for i in range(4)])


def other_core(value):
    return lax.ppermute(value, "c", [(0, 1), (1, 0)])


def vmem(count):
    return [pl.BlockSpec(memory_space=pltpu.VMEM)] * count


def hbm(count):
    return [pl.BlockSpec(memory_space=pltpu.HBM)] * count


def small(kernel, outs, *operands):
    return pl.pallas_call(
        kernel,
        out_shape=[jax.ShapeDtypeStruct(shape, BF16) for shape in outs],
        in_specs=vmem(len(operands)),
        out_specs=vmem(len(outs)),
        compiler_params=pltpu.CompilerParams(vmem_limit_bytes=4 << 20),
    )(*operands)


def moved(shape, source_of, *blocks):
    joined = jnp.concatenate([b[...] for b in blocks], axis=0)
    row = lax.broadcasted_iota(jnp.int32, (shape[0], joined.shape[0]), 0)
    column = lax.broadcasted_iota(jnp.int32, (shape[0], joined.shape[0]), 1)
    source, valid = source_of(row)
    picks = jnp.where((source == column) & valid, 1.0, 0.0).astype(BF16)
    return jnp.dot(picks, joined, preferred_element_type=F32)


def slots_of(ids):
    tokens = ids.shape[1]
    slot = lax.broadcasted_iota(jnp.int32, (ROWS, tokens), 0)
    k = (slot * 3641) >> 16
    inside = slot - k * CAP
    zh, y2 = lax.axis_index("zh"), lax.axis_index("y2")
    expert = ((zh + k) & 3) * 2 + (y2 ^ (k >> 2))
    first, second = ids[0:1, :] == expert, ids[1:2, :] == expert
    routed = jnp.where(first | second, 1.0, 0.0).astype(BF16)
    earlier = lax.broadcasted_iota(jnp.int32, (tokens, tokens), 0) < lax.broadcasted_iota(
        jnp.int32, (tokens, tokens), 1
    )
    before = jnp.dot(
        routed, jnp.where(earlier, 1.0, 0.0).astype(BF16), preferred_element_type=F32
    )
    here = before == inside.astype(F32)
    return first & here, second & here


def select_kernel(ids_ref, tokens_ref, keep_ref, send_ref):
    first, second = slots_of(ids_ref[...])
    picks = jnp.where(first | second, 1.0, 0.0).astype(BF16)
    chosen = jnp.dot(picks, tokens_ref[...], preferred_element_type=F32).astype(BF16)
    keep_ref[...] = chosen[:KEPT]
    send_ref[...] = chosen[KEPT:]


def in_blocks(row):
    block = (row * 1639) >> 16
    inside = row - block * BLOCK
    half = jnp.where(inside < CAP, 0, 1)
    return block, inside, half


def shuffle_kernel(keep_ref, came_ref, *out_refs):
    def source_of(row):
        block, inside, half = in_blocks(row)
        return half * KEPT + block * CAP + inside - half * CAP, inside < 2 * CAP

    rows = moved((FAR * BLOCK, 0), source_of, keep_ref, came_ref)
    for k, out in enumerate(out_refs):
        out[...] = rows[k * BLOCK : (k + 1) * BLOCK].astype(BF16)


def pack_kernel(*refs):
    *blocks, sums_ref, out_ref = refs

    def source_of(row):
        block = (row * 1821) >> 16
        return block * BLOCK + row - block * 2 * CAP, row >= 0

    out_ref[:ROWS] = moved((ROWS, 0), source_of, *blocks).astype(BF16)
    out_ref[ROWS:] = sums_ref[...]


def unpack_kernel(*refs):
    terms, out_refs = refs[:FAR], refs[FAR:]
    total = sum(t[...].astype(F32) for t in terms).astype(BF16)

    def source_of(row):
        block, inside, _ = in_blocks(row)
        return block * 2 * CAP + inside, inside < 2 * CAP

    rows = moved((FAR * BLOCK, 0), source_of, total)
    for k, out in enumerate(out_refs):
        out[...] = rows[k * BLOCK : (k + 1) * BLOCK].astype(BF16)


def unshuffle_kernel(*refs):
    blocks, (keep_ref, send_ref) = refs[:FAR], refs[FAR:]

    def source_of(row):
        k = (row * 3641) >> 16
        return (k & 3) * BLOCK + (k >> 2) * CAP + row - k * CAP, row >= 0

    rows = moved((ROWS, 0), source_of, *blocks).astype(BF16)
    keep_ref[...] = rows[:KEPT]
    send_ref[...] = rows[KEPT:]


def transposed_dot(left, right):
    return lax.dot_general(left, right, (((1,), (1,)), ((), ())), preferred_element_type=F32)


def halves(value):
    high = value.astype(BF16)
    return high, (value - high.astype(F32)).astype(BF16)


def stats_kernel(tokens_ref, gain_ref, router_ref, out_ref):
    tokens, width = tokens_ref.shape
    part = lax.axis_index("zl") * 4 + lax.axis_index("x")
    here = pl.ds(pl.multiple_of(part * width, width), width)
    values = tokens_ref[...].astype(F32)
    router = router_ref[:, here]
    ones = jnp.ones_like(router)
    scaled, squares = halves(values * gain_ref[:, here]), halves(values * values)
    out_ref[...] = jnp.zeros_like(out_ref)
    for n, (left, terms) in enumerate(((router, scaled), (ones, squares))):
        for k, v in enumerate(halves(sum(transposed_dot(left, t) for t in terms))):
            start = (2 * n + k) * 128
            out_ref[:, start : start + tokens] = v


def stats_in(tile, tokens):
    parts = [tile[ROWS:, n * 128 : n * 128 + tokens].astype(F32) for n in range(4)]
    return parts[0] + parts[1], parts[2] + parts[3]


def combine_kernel(width_all, ids_ref, sums_ref, keep_ref, came_ref, out_ref):
    ids = ids_ref[...]
    sums = sums_ref[...]
    experts = sums.shape[0] // 2
    scale = lax.rsqrt(sums[experts : experts + 1] / width_all + EPSILON)
    named = lax.broadcasted_iota(jnp.int32, (experts, ids.shape[1]), 0)
    logits = [
        jnp.sum(jnp.where(named == ids[k : k + 1], sums[:experts], 0.0), axis=0, keepdims=True)
        * scale
        for k in (0, 1)
    ]
    gate_first = 1.0 / (1.0 + jnp.exp(logits[1] - logits[0]))
    gate_second = 1.0 / (1.0 + jnp.exp(logits[0] - logits[1]))
    first, second = slots_of(ids)
    weights = jnp.where(first, gate_first, 0.0) + jnp.where(second, gate_second, 0.0)
    rows = jnp.concatenate([keep_ref[...], came_ref[...]], axis=0)
    out_ref[...] = sum(
        lax.dot_general(w, rows, (((0,), (0,)), ((), ())), preferred_element_type=F32)
        for w in halves(weights)
    ).astype(BF16)


def offset_place(square, ring):
    step = jnp.where(ring == 1, 3, jnp.where(ring == 2, 1, jnp.where(ring == 3, 2, 0)))
    feature = (lax.axis_index("zl") ^ (square >> 1)) * 4 + ((lax.axis_index("x") + step) & 3)
    return square & 1, feature


def tile_place(outer, inner):
    core = lax.axis_index("c")
    return offset_place(jnp.where(core == 0, outer, inner), jnp.where(core == 0, inner, outer))


CHUNK = 16


def in_hbm(*arrays):
    return [pltpu.with_memory_space_constraint(a, pltpu.HBM) for a in arrays]


def hidden_kernel(width_all, gain_ref, *refs):
    tiles, others, owns = refs[:16], refs[16:18], refs[18:20]
    out_ref, sums_ref, x_ref, w_ref, squares_ref, sems = refs[20:]
    copies = [pltpu.make_async_copy(w, w_ref.at[n], sems.at[n]) for n, w in enumerate(owns)]
    for copy in copies:
        copy.start()
    rows, width = ROWS, tiles[0].shape[1]
    slices = w_ref.shape[2]
    experts, tokens = sums_ref.shape[0] // 2, sums_ref.shape[1]
    squares_ref[...] = jnp.zeros_like(squares_ref)
    sums_ref[...] = jnp.zeros_like(sums_ref)
    for index, tile in enumerate(tiles):
        row_class, feature = tile_place(index // 4, index % 4)
        column_at = pl.ds(pl.multiple_of(feature * width, width), width)
        gain = gain_ref[:, column_at]

        def prepare(n, _, tile=tile, row_class=row_class, column_at=column_at, gain=gain):
            row_at = pl.ds(pl.multiple_of(row_class * rows + n * CHUNK, CHUNK), CHUNK)
            values = tile[pl.ds(pl.multiple_of(n * CHUNK, CHUNK), CHUNK), :].astype(F32)
            x_ref[row_at, column_at] = (values * gain).astype(BF16)
            square = values * values
            squares_ref[row_at, :] += sum(
                square[:, j * 128 : (j + 1) * 128] for j in range(width // 128)
            )
            return 0

        lax.fori_loop(0, rows // CHUNK, prepare, 0)
        own = jnp.where(row_class == 0, 1.0, 0.0)
        logits, squares = stats_in(tile, tokens)
        sums_ref[:experts] += logits * own
        sums_ref[experts:] += squares * own
    scale = lax.rsqrt(jnp.sum(squares_ref[...], axis=1, keepdims=True) / width_all + EPSILON)

    def give(start, gate_weight, up_weight):
        gate = jnp.dot(x_ref[...], gate_weight[...], preferred_element_type=F32) * scale
        up = jnp.dot(x_ref[...], up_weight[...], preferred_element_type=F32) * scale
        out_ref[:, start : start + slices] = (gate * (1.0 / (1.0 + jnp.exp(-gate))) * up).astype(
            BF16
        )

    give(slices, *others)
    for copy in copies:
        copy.wait()
    give(0, w_ref.at[0], w_ref.at[1])


def hidden_of(gain, tiles, others, owns, sums_shape):
    rows = ROWS
    width_all, slices = owns[0].shape
    return pl.pallas_call(
        partial(hidden_kernel, width_all),
        out_shape=[
            jax.ShapeDtypeStruct((2 * rows, 2 * slices), BF16),
            jax.ShapeDtypeStruct(sums_shape, F32),
        ],
        in_specs=vmem(19) + hbm(2),
        out_specs=vmem(2),
        scratch_shapes=[
            pltpu.VMEM((2 * rows, width_all), BF16),
            pltpu.VMEM((2, width_all, slices), BF16),
            pltpu.VMEM((2 * rows, 128), F32),
            pltpu.SemaphoreType.DMA((2,)),
        ],
        compiler_params=pltpu.CompilerParams(vmem_limit_bytes=20 << 20),
        cost_estimate=pl.CostEstimate(
            flops=2 * 2 * rows * width_all * 4 * slices,
            bytes_accessed=4 * width_all * slices * 2,
            transcendentals=0,
        ),
        name="hidden",
    )(gain, *tiles, *others, *in_hbm(*owns))


def down_kernel(places, hidden_ref, own_ref, other_ref, *refs):
    out_refs, y_ref = refs[:-1], refs[-1]
    slices = own_ref.shape[0]
    rows, width = y_ref.shape[1] // 2, y_ref.shape[2]

    def step(n, _):
        _, feature = offset_place((n >> 2) * 2, n & 3)
        column_at = pl.ds(pl.multiple_of(feature * width, width), width)
        y_ref[n] = (
            jnp.dot(hidden_ref[:, :slices], own_ref[:, column_at], preferred_element_type=F32)
            + jnp.dot(hidden_ref[:, slices:], other_ref[:, column_at], preferred_element_type=F32)
        ).astype(BF16)
        return 0

    lax.fori_loop(0, 8, step, 0)
    core = lax.axis_index("c")

    def give(which):
        for n in range(8):
            for row_class in range(2):
                square, ring = (n >> 2) * 2 + row_class, n & 3
                outer, inner = (square, ring) if which == 0 else (ring, square)
                at, start = places[outer * 4 + inner]
                out_refs[at][start : start + rows, :] = y_ref[
                    n, row_class * rows : (row_class + 1) * rows, :
                ]

    @pl.when(core == 0)
    def _():
        give(0)

    @pl.when(core == 1)
    def _():
        give(1)


def down_of(shapes, places, hidden, own, other):
    slices, width_all = own.shape
    width = width_all // 8
    return pl.pallas_call(
        partial(down_kernel, places),
        out_shape=[jax.ShapeDtypeStruct((rows, width), BF16) for rows in shapes],
        in_specs=vmem(3),
        out_specs=vmem(len(shapes)),
        scratch_shapes=[pltpu.VMEM((8, hidden.shape[0], width), BF16)],
        compiler_params=pltpu.CompilerParams(vmem_limit_bytes=20 << 20),
        cost_estimate=pl.CostEstimate(
            flops=2 * hidden.shape[0] * width_all * 2 * slices,
            bytes_accessed=2 * slices * width_all * 2,
            transcendentals=0,
        ),
        name="down",
    )(hidden, own, other)


def added_kernel(starts, *refs):
    *terms, out_ref = refs
    rows = out_ref.shape[0]
    out_ref[...] = sum(t[n : n + rows, :].astype(F32) for t, n in zip(terms, starts)).astype(BF16)


def added(*terms):
    terms = [t if isinstance(t, tuple) else (t, 0) for t in terms]
    (out,) = small(
        partial(added_kernel, [n for _, n in terms]),
        [(ROWS, terms[0][0].shape[1])],
        *(t for t, _ in terms),
    )
    return out


def per_device(tokens, norm_gain, router_weight, expert_ids, gate_proj, up_proj, down_proj):
    width_all = router_weight.shape[0]
    width = tokens.shape[1]
    gain = norm_gain.reshape(1, width_all)
    ids = expert_ids.T
    kept, block = (KEPT, width), (BLOCK, width)

    keep, send = small(select_kernel, [kept, kept], ids, tokens)
    came = across_y(send)
    blocks = small(shuffle_kernel, [block] * FAR, keep, came)
    arrived = [blocks[0]] + [along_z(blocks[k], k) for k in (1, 2, 3)]
    gate_other = other_core(gate_proj)
    up_other = other_core(up_proj)
    down_other = other_core(down_proj)
    (part_sums,) = small(stats_kernel, [(EXTRA, width)], tokens, gain, router_weight.T)
    (mine,) = small(pack_kernel, [(ROWS + EXTRA, width)], *arrived, part_sums)

    inner = [mine, hop(mine, "x+", "y"), hop(mine, "x-", "z"), hop(mine, "xx", "yz")]
    outer = [inner, [], [], [None] * 4]
    for a in range(4):
        outer[1].append(hop(inner[a], "y", "x+"))
        outer[2].append(hop(inner[a], "z", "x-"))
    for a in (0, 1):
        outer[3][a] = hop(outer[1][a], "z", "x+")
    for a in (2, 3):
        outer[3][a] = hop(outer[2][a], "y", "x-")
    tiles = [outer[m][a] for m in range(4) for a in range(4)]
    sums_shape = (2 * router_weight.shape[1], tokens.shape[0])
    hidden, sums = hidden_of(
        gain, tiles, (gate_other, up_other), (gate_proj, up_proj), sums_shape
    )

    shapes = [ROWS] * 12 + [2 * ROWS] * 2
    places = {4 * 0 + a: (a, 0) for a in range(4)}
    places |= {4 * 3 + a: (4 + a, 0) for a in range(4)}
    places |= {4 * 1 + 0: (8, 0), 4 * 1 + 1: (9, 0), 4 * 2 + 2: (10, 0), 4 * 2 + 3: (11, 0)}
    places |= {4 * 1 + 2: (12, 0), 4 * 1 + 3: (12, ROWS), 4 * 2 + 0: (13, 0), 4 * 2 + 1: (13, ROWS)}
    part = down_of(shapes, places, hidden, down_proj, down_other)
    own, far, near, pairs = part[:4], part[4:8], part[8:12], part[12:]
    ways = [("z", "x-"), ("z", "x-"), ("y", "x+"), ("y", "x+")]
    far_in = [hop(far[n], *ways[n]) for n in range(4)]
    first = hop(pairs[0], "y", "x-")
    second = hop(pairs[1], "z", "x+")
    ways = [("y", "x-"), ("y", "x-"), ("z", "x+"), ("z", "x+")]
    near_in = [hop(added(near[n], far_in[n]), *ways[n]) for n in range(4)]
    in_pairs = [(second, 0), (second, ROWS), (first, 0), (first, ROWS)]
    total = [added(own[n], near_in[n], in_pairs[n]) for n in range(4)]
    terms = [
        total[0], hop(total[1], "x-", "y"), hop(total[2], "x+", "z"), hop(total[3], "xx", "yz")
    ]
    blocks = small(unpack_kernel, [block] * FAR, *terms)
    back = [blocks[0]] + [along_z(blocks[k], FAR - k) for k in (1, 2, 3)]
    keep, send = small(unshuffle_kernel, [kept, kept], *back)
    came = across_y(send)
    return pl.pallas_call(
        partial(combine_kernel, width_all),
        out_shape=jax.ShapeDtypeStruct(tokens.shape, BF16),
        in_specs=vmem(4),
        out_specs=vmem(1)[0],
        compiler_params=pltpu.CompilerParams(vmem_limit_bytes=4 << 20),
        name="combine",
    )(ids, sums, keep, came)


def solution(mesh):
    cut = Mesh(mesh.devices.reshape(SIZES), AXES)
    split = GRP + TP
    placed = (
        P(GRP, TP),
        P(),
        P(),
        P(GRP, None),
        P(None, split),
        P(None, split),
        P(split, None),
    )

    return jax.shard_map(per_device, mesh=cut, in_specs=placed, out_specs=P(GRP, TP), check_vma=False)
```

```python
from functools import partial

import jax
import jax.numpy as jnp
from jax import lax
from jax.experimental import pallas as pl
from jax.experimental.pallas import tpu as pltpu
from jax.sharding import Mesh
from jax.sharding import PartitionSpec as P


AXES = ("zh", "y2", "y1", "c", "zl", "x")
SIZES = (4, 2, 2, 2, 2, 4)
GRP = ("zh", "y2", "y1", "c")
TP = ("zl", "x")
OWNER = ("y1", "c", "zl", "x")
CAP = 18
FAR = 4
KEPT = FAR * CAP
ROWS = 2 * KEPT
EXTRA = 8
BLOCK = 40
EPSILON = 1e-05
F32 = jnp.float32
BF16 = jnp.bfloat16


def place(y, z, x, step):
    if step == "x+":
        return y, z, (x + 1) % 4
    if step == "x-":
        return y, z, (x - 1) % 4
    if step == "xx":
        return y, z, (x + 2) % 4
    if step == "y":
        return 1 - y, z, x
    if step == "z":
        return y, 1 - z, x
    return 1 - y, 1 - z, x


def owner_pairs(step_core0, step_core1):
    pairs = []
    for y in range(2):
        for core, step in enumerate((step_core0, step_core1)):
            for z in range(2):
                for x in range(4):
                    y_to, z_to, x_to = place(y, z, x, step)
                    source = ((y * 2 + core) * 2 + z) * 4 + x
                    target = ((y_to * 2 + core) * 2 + z_to) * 4 + x_to
                    pairs.append((source, target))
    return pairs


def hop(value, step_core0, step_core1):
    return lax.ppermute(value, OWNER, owner_pairs(step_core0, step_core1))


def along_z(value, distance):
    return lax.ppermute(value, "zh", [(i, (i + distance) % FAR) for i in range(FAR)])


def across_y(value):
    return lax.ppermute(value, ("y2", "y1"), [(i, 3 - i) for i in range(4)])


def other_core(value):
    return lax.ppermute(value, "c", [(0, 1), (1, 0)])


def vmem(count):
    return [pl.BlockSpec(memory_space=pltpu.VMEM)] * count


def hbm(count):
    return [pl.BlockSpec(memory_space=pltpu.HBM)] * count


def in_hbm(*arrays):
    return [pltpu.with_memory_space_constraint(a, pltpu.HBM) for a in arrays]


def small(kernel, outs, *operands):
    return pl.pallas_call(
        kernel,
        out_shape=[jax.ShapeDtypeStruct(shape, BF16) for shape in outs],
        in_specs=vmem(len(operands)),
        out_specs=vmem(len(outs)),
        compiler_params=pltpu.CompilerParams(vmem_limit_bytes=4 << 20),
    )(*operands)


def moved(shape, source_of, *blocks):
    joined = jnp.concatenate([b[...] for b in blocks], axis=0)
    row = lax.broadcasted_iota(jnp.int32, (shape[0], joined.shape[0]), 0)
    column = lax.broadcasted_iota(jnp.int32, (shape[0], joined.shape[0]), 1)
    source, valid = source_of(row)
    picks = jnp.where((source == column) & valid, 1.0, 0.0).astype(BF16)
    return jnp.dot(picks, joined, preferred_element_type=F32)


def slots_of(ids):
    tokens = ids.shape[1]
    slot = lax.broadcasted_iota(jnp.int32, (ROWS, tokens), 0)
    k = (slot * 3641) >> 16
    inside = slot - k * CAP
    zh, y2 = lax.axis_index("zh"), lax.axis_index("y2")
    expert = ((zh + k) & 3) * 2 + (y2 ^ (k >> 2))
    first, second = ids[0:1, :] == expert, ids[1:2, :] == expert
    routed = jnp.where(first | second, 1.0, 0.0).astype(BF16)
    earlier = lax.broadcasted_iota(jnp.int32, (tokens, tokens), 0) < lax.broadcasted_iota(
        jnp.int32, (tokens, tokens), 1
    )
    before = jnp.dot(
        routed, jnp.where(earlier, 1.0, 0.0).astype(BF16), preferred_element_type=F32
    )
    here = before == inside.astype(F32)
    return first & here, second & here


def select_kernel(ids_hbm, tokens_hbm, keep_ref, send_ref, ids_ref, tokens_ref, sems):
    fetch = pltpu.make_async_copy(ids_hbm, ids_ref, sems.at[0])
    fetch_tokens = pltpu.make_async_copy(tokens_hbm, tokens_ref, sems.at[1])
    fetch.start()
    fetch_tokens.start()
    fetch.wait()
    first, second = slots_of(ids_ref[...])
    picks = jnp.where(first | second, 1.0, 0.0).astype(BF16)
    fetch_tokens.wait()
    chosen = jnp.dot(picks, tokens_ref[...], preferred_element_type=F32).astype(BF16)
    keep_ref[...] = chosen[:KEPT]
    send_ref[...] = chosen[KEPT:]


def select(ids, tokens):
    kept = jax.ShapeDtypeStruct((KEPT, tokens.shape[1]), BF16)
    return pl.pallas_call(
        select_kernel,
        out_shape=[kept, kept],
        in_specs=hbm(2),
        out_specs=vmem(2),
        scratch_shapes=[
            pltpu.VMEM(ids.shape, ids.dtype),
            pltpu.VMEM(tokens.shape, BF16),
            pltpu.SemaphoreType.DMA((2,)),
        ],
        compiler_params=pltpu.CompilerParams(vmem_limit_bytes=4 << 20),
        name="select",
    )(*in_hbm(ids, tokens))


def in_blocks(row):
    block = (row * 1639) >> 16
    inside = row - block * BLOCK
    half = jnp.where(inside < CAP, 0, 1)
    return block, inside, half


def shuffle_kernel(keep_ref, came_ref, *out_refs):
    def source_of(row):
        block, inside, half = in_blocks(row)
        return half * KEPT + block * CAP + inside - half * CAP, inside < 2 * CAP

    rows = moved((FAR * BLOCK, 0), source_of, keep_ref, came_ref)
    for k, out in enumerate(out_refs):
        out[...] = rows[k * BLOCK : (k + 1) * BLOCK].astype(BF16)


def pack_kernel(*refs):
    *blocks, sums_ref, out_ref = refs

    def source_of(row):
        block = (row * 1821) >> 16
        return block * BLOCK + row - block * 2 * CAP, row >= 0

    out_ref[:ROWS] = moved((ROWS, 0), source_of, *blocks).astype(BF16)
    out_ref[ROWS:] = sums_ref[...]


def unpack_kernel(*refs):
    terms, out_refs = refs[:FAR], refs[FAR:]
    total = sum(t[...].astype(F32) for t in terms).astype(BF16)

    def source_of(row):
        block, inside, _ = in_blocks(row)
        return block * 2 * CAP + inside, inside < 2 * CAP

    rows = moved((FAR * BLOCK, 0), source_of, total)
    for k, out in enumerate(out_refs):
        out[...] = rows[k * BLOCK : (k + 1) * BLOCK].astype(BF16)


def unshuffle_kernel(*refs):
    blocks, (keep_ref, send_ref) = refs[:FAR], refs[FAR:]

    def source_of(row):
        k = (row * 3641) >> 16
        return (k & 3) * BLOCK + (k >> 2) * CAP + row - k * CAP, row >= 0

    rows = moved((ROWS, 0), source_of, *blocks).astype(BF16)
    keep_ref[...] = rows[:KEPT]
    send_ref[...] = rows[KEPT:]


def transposed_dot(left, right):
    return lax.dot_general(left, right, (((1,), (1,)), ((), ())), preferred_element_type=F32)


def halves(value):
    high = value.astype(BF16)
    return high, (value - high.astype(F32)).astype(BF16)


def stats_kernel(tokens_hbm, gain_hbm, router_hbm, out_ref, gain_ref, tokens_ref, router_ref, sems):
    tokens, width = tokens_ref.shape
    part = lax.axis_index("zl") * 4 + lax.axis_index("x")
    here = pl.ds(pl.multiple_of(part * width, width), width)
    ways = ((tokens_hbm, tokens_ref), (gain_hbm, gain_ref), (router_hbm.at[:, here], router_ref))
    fetches = [pltpu.make_async_copy(a, b, sems.at[n]) for n, (a, b) in enumerate(ways)]
    for fetch in fetches:
        fetch.start()
    out_ref[...] = jnp.zeros_like(out_ref)
    for fetch in fetches:
        fetch.wait()
    values = tokens_ref[...].astype(F32)
    router = router_ref[...]
    ones = jnp.ones_like(router)
    scaled, squares = halves(values * gain_ref[:, here]), halves(values * values)
    for n, (left, terms) in enumerate(((router, scaled), (ones, squares))):
        for k, v in enumerate(halves(sum(transposed_dot(left, t) for t in terms))):
            start = (2 * n + k) * 128
            out_ref[:, start : start + tokens] = v


def stats(tokens, gain, router):
    width = tokens.shape[1]
    return pl.pallas_call(
        stats_kernel,
        out_shape=[
            jax.ShapeDtypeStruct((EXTRA, width), BF16),
            jax.ShapeDtypeStruct(gain.shape, F32),
        ],
        in_specs=hbm(3),
        out_specs=vmem(2),
        scratch_shapes=[
            pltpu.VMEM(tokens.shape, BF16),
            pltpu.VMEM((router.shape[0], width), BF16),
            pltpu.SemaphoreType.DMA((3,)),
        ],
        compiler_params=pltpu.CompilerParams(vmem_limit_bytes=4 << 20),
        name="stats",
    )(*in_hbm(tokens, gain, router))


def stats_in(tile, tokens):
    parts = [tile[ROWS:, n * 128 : n * 128 + tokens].astype(F32) for n in range(4)]
    return parts[0] + parts[1], parts[2] + parts[3]


def combine_kernel(width_all, ids_ref, sums_ref, keep_ref, came_ref, out_ref):
    ids = ids_ref[...]
    sums = sums_ref[...]
    experts = sums.shape[0] // 2
    scale = lax.rsqrt(sums[experts : experts + 1] / width_all + EPSILON)
    named = lax.broadcasted_iota(jnp.int32, (experts, ids.shape[1]), 0)
    logits = [
        jnp.sum(jnp.where(named == ids[k : k + 1], sums[:experts], 0.0), axis=0, keepdims=True)
        * scale
        for k in (0, 1)
    ]
    gate_first = 1.0 / (1.0 + jnp.exp(logits[1] - logits[0]))
    gate_second = 1.0 / (1.0 + jnp.exp(logits[0] - logits[1]))
    first, second = slots_of(ids)
    weights = jnp.where(first, gate_first, 0.0) + jnp.where(second, gate_second, 0.0)
    rows = jnp.concatenate([keep_ref[...], came_ref[...]], axis=0)
    out_ref[...] = sum(
        lax.dot_general(w, rows, (((0,), (0,)), ((), ())), preferred_element_type=F32)
        for w in halves(weights)
    ).astype(BF16)


def offset_place(square, ring):
    step = jnp.where(ring == 1, 3, jnp.where(ring == 2, 1, jnp.where(ring == 3, 2, 0)))
    feature = (lax.axis_index("zl") ^ (square >> 1)) * 4 + ((lax.axis_index("x") + step) & 3)
    return square & 1, feature


def tile_place(outer, inner):
    core = lax.axis_index("c")
    return offset_place(jnp.where(core == 0, outer, inner), jnp.where(core == 0, inner, outer))


CHUNK = 16
EARLY = 12


def prepare(tile, gain, out_ref, row_start, column_at, squares_ref, squares_start):
    width = tile.shape[1]

    def step(n, _):
        at = pl.multiple_of(n * CHUNK, CHUNK)
        values = tile[pl.ds(at, CHUNK), :].astype(F32)
        row_at = pl.ds(pl.multiple_of(row_start + at, CHUNK), CHUNK)
        out_ref[row_at, column_at] = (values * gain).astype(BF16)
        square = values * values
        squares_at = pl.ds(pl.multiple_of(squares_start + at, CHUNK), CHUNK)
        squares_ref[squares_at, :] += sum(
            square[:, j * 128 : (j + 1) * 128] for j in range(width // 128)
        )
        return 0

    lax.fori_loop(0, ROWS // CHUNK, step, 0)


def add_stats(tile, row_class, sums_ref):
    experts, tokens = sums_ref.shape[0] // 2, sums_ref.shape[1]
    own = jnp.where(row_class == 0, 1.0, 0.0)
    logits, squares = stats_in(tile, tokens)
    sums_ref[:experts] += logits * own
    sums_ref[experts:] += squares * own


def columns_of(feature, width):
    return pl.ds(pl.multiple_of(feature * width, width), width)


def early_kernel(gain_ref, *refs):
    tiles, others, owns = refs[:EARLY], refs[EARLY : EARLY + 2], refs[EARLY + 2 : EARLY + 5]
    acc_ref, squares_ref, sums_ref, *own_refs, x_ref, sems = refs[EARLY + 5 :]
    copies = [
        pltpu.make_async_copy(a, b, sems.at[n]) for n, (a, b) in enumerate(zip(owns, own_refs))
    ]
    for copy in copies:
        copy.start()
    width = tiles[0].shape[1]
    squares_ref[...] = jnp.zeros_like(squares_ref)
    sums_ref[...] = jnp.zeros_like(sums_ref)
    for index in range(16):
        row_class, feature = tile_place(index // 4, index % 4)
        column_at = columns_of(feature, width)
        start = row_class * ROWS
        if index < EARLY:
            gain = gain_ref[:, column_at]
            prepare(tiles[index], gain, x_ref, start, column_at, squares_ref, start)
            add_stats(tiles[index], row_class, sums_ref)
        else:
            row_at = pl.ds(pl.multiple_of(start, ROWS), ROWS)
            x_ref[row_at, column_at] = jnp.zeros((ROWS, width), BF16)
    for n, weight in enumerate((*others, *own_refs[:2])):
        if n >= 2:
            copies[n - 2].wait()
        acc_ref[n] = jnp.dot(x_ref[...], weight[...], preferred_element_type=F32)
    copies[2].wait()


def early_of(gain, tiles, others, owns, sums_shape):
    width_all, slices = owns[0].shape
    return pl.pallas_call(
        early_kernel,
        out_shape=[
            jax.ShapeDtypeStruct((4, 2 * ROWS, slices), F32),
            jax.ShapeDtypeStruct((2 * ROWS, 128), F32),
            jax.ShapeDtypeStruct(sums_shape, F32),
            *(jax.ShapeDtypeStruct(w.shape, BF16) for w in owns),
        ],
        in_specs=vmem(EARLY + 3) + hbm(3),
        out_specs=vmem(6),
        scratch_shapes=[
            pltpu.VMEM((2 * ROWS, width_all), BF16),
            pltpu.SemaphoreType.DMA((3,)),
        ],
        compiler_params=pltpu.CompilerParams(vmem_limit_bytes=20 << 20),
        cost_estimate=pl.CostEstimate(
            flops=2 * 2 * ROWS * width_all * 4 * slices,
            bytes_accessed=2 * width_all * slices * 2,
            transcendentals=0,
        ),
        name="early",
    )(gain, *tiles, *others, *in_hbm(*owns))


def late_kernel(width_all, gain_ref, *refs):
    tiles, weights, refs = refs[:4], refs[4:8], refs[8:]
    _, squares_in, sums_in, out_ref, sums_ref, acc_ref, squares_ref, x_ref = refs
    width = tiles[0].shape[1]
    slices = weights[0].shape[1]
    squares_ref[...] = squares_in[...]
    sums_ref[...] = sums_in[...]
    for index, tile in enumerate(tiles):
        row_class, feature = tile_place(3, index)
        column_at = columns_of(feature, width)
        start = row_class * ROWS
        gain = gain_ref[:, column_at]
        prepare(tile, gain, x_ref, 0, slice(None), squares_ref, start)
        add_stats(tile, row_class, sums_ref)
        row_at = pl.ds(pl.multiple_of(start, ROWS), ROWS)
        for n, weight in enumerate(weights):
            acc_ref[n, row_at, :] = acc_ref[n, row_at, :] + jnp.dot(
                x_ref[...], weight[column_at, :], preferred_element_type=F32
            )
    scale = lax.rsqrt(jnp.sum(squares_ref[...], axis=1, keepdims=True) / width_all + EPSILON)
    for half in range(2):
        gate, up = acc_ref[2 * half] * scale, acc_ref[2 * half + 1] * scale
        start = (1 - half) * slices
        out_ref[:, start : start + slices] = (gate * (1.0 / (1.0 + jnp.exp(-gate))) * up).astype(
            BF16
        )


def late_of(gain, tiles, weights, acc, squares, sums):
    width_all, slices = weights[0].shape
    width = tiles[0].shape[1]
    return pl.pallas_call(
        partial(late_kernel, width_all),
        out_shape=[
            jax.ShapeDtypeStruct((2 * ROWS, 2 * slices), BF16),
            jax.ShapeDtypeStruct(sums.shape, F32),
            jax.ShapeDtypeStruct(acc.shape, F32),
        ],
        in_specs=vmem(12),
        out_specs=vmem(3),
        input_output_aliases={9: 2},
        scratch_shapes=[
            pltpu.VMEM(squares.shape, F32),
            pltpu.VMEM((ROWS, width), BF16),
        ],
        compiler_params=pltpu.CompilerParams(vmem_limit_bytes=12 << 20),
        cost_estimate=pl.CostEstimate(
            flops=2 * 4 * ROWS * width * 4 * slices,
            bytes_accessed=acc.size * 8,
            transcendentals=0,
        ),
        name="late",
    )(gain, *tiles, *weights, acc, squares, sums)[:2]


def down_kernel(far, places, hidden_ref, own_ref, other_ref, *refs):
    out_refs, y_ref = refs[:-1], refs[-1]
    slices = own_ref.shape[0]
    width = y_ref.shape[2]
    core = lax.axis_index("c")

    def product(rows, square, ring):
        _, feature = offset_place(square, ring)
        column_at = columns_of(feature, width)
        return (
            jnp.dot(hidden_ref[rows, :slices], own_ref[:, column_at], preferred_element_type=F32)
            + jnp.dot(hidden_ref[rows, slices:], other_ref[:, column_at], preferred_element_type=F32)
        ).astype(BF16)

    both, first, last = slice(None), slice(0, ROWS), slice(ROWS, 2 * ROWS)

    @pl.when(core == 0)
    def _():
        def step(ring, _):
            if far:
                y_ref[ring] = product(last, 3, ring)
                return 0
            pair = product(both, 0, ring)
            y_ref[ring] = pair[:ROWS]
            y_ref[4 + ring] = pair[ROWS:]
            y_ref[8 + ring] = product(first, 2, ring)
            return 0

        lax.fori_loop(0, 4, step, 0)

    @pl.when(core == 1)
    def _():
        def step(n, _):
            ring, square = (3, 2 * n) if far else (n >> 1, 2 * (n & 1))
            pair = product(both, square, ring)
            at = square if far else 4 * ring + square
            y_ref[at] = pair[:ROWS]
            y_ref[at + 1] = pair[ROWS:]
            return 0

        lax.fori_loop(0, 2 if far else 6, step, 0)

    for index, (at, start) in enumerate(places):
        out_refs[at][start : start + ROWS, :] = y_ref[index]


def down_of(far, shapes, places, hidden, own, other):
    slices, width_all = own.shape
    width = width_all // 8
    return pl.pallas_call(
        partial(down_kernel, far, places),
        out_shape=[jax.ShapeDtypeStruct((rows, width), BF16) for rows in shapes],
        in_specs=vmem(3),
        out_specs=vmem(len(shapes)),
        scratch_shapes=[pltpu.VMEM((len(places), ROWS, width), BF16)],
        compiler_params=pltpu.CompilerParams(vmem_limit_bytes=16 << 20),
        cost_estimate=pl.CostEstimate(
            flops=2 * len(places) * ROWS * width * 2 * slices,
            bytes_accessed=2 * slices * width_all * 2,
            transcendentals=0,
        ),
        name="far" if far else "rest",
    )(hidden, own, other)


def added_kernel(starts, *refs):
    *terms, out_ref = refs
    rows = out_ref.shape[0]
    out_ref[...] = sum(t[n : n + rows, :].astype(F32) for t, n in zip(terms, starts)).astype(BF16)


def added(*terms):
    terms = [t if isinstance(t, tuple) else (t, 0) for t in terms]
    (out,) = small(
        partial(added_kernel, [n for _, n in terms]),
        [(ROWS, terms[0][0].shape[1])],
        *(t for t, _ in terms),
    )
    return out


def per_device(tokens, norm_gain, router_weight, expert_ids, gate_proj, up_proj, down_proj):
    width_all = router_weight.shape[0]
    width = tokens.shape[1]
    gain = norm_gain.reshape(1, width_all)
    ids = expert_ids.T
    kept, block = (KEPT, width), (BLOCK, width)

    keep, send = select(ids, tokens)
    came = across_y(send)
    blocks = small(shuffle_kernel, [block] * FAR, keep, came)
    arrived = [blocks[0]] + [along_z(blocks[k], k) for k in (1, 2, 3)]
    gate_other = other_core(gate_proj)
    up_other = other_core(up_proj)
    down_other = other_core(down_proj)
    part_sums, gain = stats(tokens, gain, router_weight.T)
    (mine,) = small(pack_kernel, [(ROWS + EXTRA, width)], *arrived, part_sums)

    inner = [mine, hop(mine, "x+", "y"), hop(mine, "x-", "z"), hop(mine, "xx", "yz")]
    outer = [inner, [], [], [None] * 4]
    for a in range(4):
        outer[1].append(hop(inner[a], "y", "x+"))
        outer[2].append(hop(inner[a], "z", "x-"))
    for a in (0, 1):
        outer[3][a] = hop(outer[1][a], "z", "x+")
    for a in (2, 3):
        outer[3][a] = hop(outer[2][a], "y", "x-")
    tiles = [outer[m][a] for m in range(4) for a in range(4)]
    sums_shape = (2 * router_weight.shape[1], tokens.shape[0])
    acc, squares, sums, gate_own, up_own, down_own = early_of(
        gain, tiles[:EARLY], (gate_other, up_other), (gate_proj, up_proj, down_proj), sums_shape
    )
    weights = (gate_other, up_other, gate_own, up_own)
    hidden, sums = late_of(gain, tiles[EARLY:], weights, acc, squares, sums)

    far = down_of(True, [ROWS] * 4, [(a, 0) for a in range(4)], hidden, down_own, down_other)
    places = [(a, 0) for a in range(4)]
    places += [(4, 0), (5, 0), (8, 0), (8, ROWS)]
    places += [(9, 0), (9, ROWS), (6, 0), (7, 0)]
    shapes = [ROWS] * 8 + [2 * ROWS] * 2
    rest = down_of(False, shapes, places, hidden, down_own, down_other)
    own, near, pairs = rest[:4], rest[4:8], rest[8:]
    ways = [("z", "x-"), ("z", "x-"), ("y", "x+"), ("y", "x+")]
    far_in = [hop(far[n], *ways[n]) for n in range(4)]
    first = hop(pairs[0], "y", "x-")
    second = hop(pairs[1], "z", "x+")
    ways = [("y", "x-"), ("y", "x-"), ("z", "x+"), ("z", "x+")]
    near_in = [hop(added(near[n], far_in[n]), *ways[n]) for n in range(4)]
    in_pairs = [(second, 0), (second, ROWS), (first, 0), (first, ROWS)]
    total = [added(own[n], near_in[n], in_pairs[n]) for n in range(4)]
    terms = [
        total[0], hop(total[1], "x-", "y"), hop(total[2], "x+", "z"), hop(total[3], "xx", "yz")
    ]
    blocks = small(unpack_kernel, [block] * FAR, *terms)
    back = [blocks[0]] + [along_z(blocks[k], FAR - k) for k in (1, 2, 3)]
    keep, send = small(unshuffle_kernel, [kept, kept], *back)
    came = across_y(send)
    return pl.pallas_call(
        partial(combine_kernel, width_all),
        out_shape=jax.ShapeDtypeStruct(tokens.shape, BF16),
        in_specs=vmem(4),
        out_specs=vmem(1)[0],
        compiler_params=pltpu.CompilerParams(vmem_limit_bytes=4 << 20),
        name="combine",
    )(ids, sums, keep, came)


def solution(mesh):
    cut = Mesh(mesh.devices.reshape(SIZES), AXES)
    split = GRP + TP
    placed = (
        P(GRP, TP),
        P(),
        P(),
        P(GRP, None),
        P(None, split),
        P(None, split),
        P(split, None),
    )

    return jax.shard_map(per_device, mesh=cut, in_specs=placed, out_specs=P(GRP, TP), check_vma=False)
```

```python
from functools import partial

import jax
import jax.numpy as jnp
from jax import lax
from jax.experimental import pallas as pl
from jax.experimental.pallas import tpu as pltpu
from jax.sharding import Mesh
from jax.sharding import PartitionSpec as P


AXES = ("zh", "y2", "y1", "c", "zl", "x")
SIZES = (4, 2, 2, 2, 2, 4)
GRP = ("zh", "y2", "y1", "c")
TP = ("zl", "x")
OWNER = ("y1", "c", "zl", "x")
CAP = 18
FAR = 4
KEPT = FAR * CAP
ROWS = 2 * KEPT
EXTRA = 8
BLOCK = 40
EPSILON = 1e-05
F32 = jnp.float32
BF16 = jnp.bfloat16


def place(y, z, x, step):
    if step == "x+":
        return y, z, (x + 1) % 4
    if step == "x-":
        return y, z, (x - 1) % 4
    if step == "xx":
        return y, z, (x + 2) % 4
    if step == "y":
        return 1 - y, z, x
    if step == "z":
        return y, 1 - z, x
    return 1 - y, 1 - z, x


def owner_pairs(step_core0, step_core1):
    pairs = []
    for y in range(2):
        for core, step in enumerate((step_core0, step_core1)):
            for z in range(2):
                for x in range(4):
                    y_to, z_to, x_to = place(y, z, x, step)
                    source = ((y * 2 + core) * 2 + z) * 4 + x
                    target = ((y_to * 2 + core) * 2 + z_to) * 4 + x_to
                    pairs.append((source, target))
    return pairs


def hop(value, step_core0, step_core1):
    return lax.ppermute(value, OWNER, owner_pairs(step_core0, step_core1))


def along_z(value, distance):
    return lax.ppermute(value, "zh", [(i, (i + distance) % FAR) for i in range(FAR)])


def across_y(value):
    return lax.ppermute(value, ("y2", "y1"), [(i, 3 - i) for i in range(4)])


def other_core(value):
    return lax.ppermute(value, "c", [(0, 1), (1, 0)])


def vmem(count):
    return [pl.BlockSpec(memory_space=pltpu.VMEM)] * count


def hbm(count):
    return [pl.BlockSpec(memory_space=pltpu.HBM)] * count


def in_hbm(*arrays):
    return [pltpu.with_memory_space_constraint(a, pltpu.HBM) for a in arrays]


def small(kernel, outs, *operands):
    return pl.pallas_call(
        kernel,
        out_shape=[jax.ShapeDtypeStruct(shape, BF16) for shape in outs],
        in_specs=vmem(len(operands)),
        out_specs=vmem(len(outs)),
        compiler_params=pltpu.CompilerParams(vmem_limit_bytes=4 << 20),
    )(*operands)


def moved(shape, source_of, *blocks):
    joined = jnp.concatenate([b[...] for b in blocks], axis=0)
    row = lax.broadcasted_iota(jnp.int32, (shape[0], joined.shape[0]), 0)
    column = lax.broadcasted_iota(jnp.int32, (shape[0], joined.shape[0]), 1)
    source, valid = source_of(row)
    picks = jnp.where((source == column) & valid, 1.0, 0.0).astype(BF16)
    return jnp.dot(picks, joined, preferred_element_type=F32)


def slots_of(ids):
    tokens = ids.shape[1]
    slot = lax.broadcasted_iota(jnp.int32, (ROWS, tokens), 0)
    k = (slot * 3641) >> 16
    inside = slot - k * CAP
    zh, y2 = lax.axis_index("zh"), lax.axis_index("y2")
    expert = ((zh + k) & 3) * 2 + (y2 ^ (k >> 2))
    first, second = ids[0:1, :] == expert, ids[1:2, :] == expert
    routed = jnp.where(first | second, 1.0, 0.0).astype(BF16)
    earlier = lax.broadcasted_iota(jnp.int32, (tokens, tokens), 0) < lax.broadcasted_iota(
        jnp.int32, (tokens, tokens), 1
    )
    before = jnp.dot(
        routed, jnp.where(earlier, 1.0, 0.0).astype(BF16), preferred_element_type=F32
    )
    here = before == inside.astype(F32)
    return first & here, second & here


def select_kernel(ids_hbm, tokens_hbm, keep_ref, send_ref, ids_ref, tokens_ref, sems):
    fetch = pltpu.make_async_copy(ids_hbm, ids_ref, sems.at[0])
    fetch_tokens = pltpu.make_async_copy(tokens_hbm, tokens_ref, sems.at[1])
    fetch.start()
    fetch_tokens.start()
    fetch.wait()
    first, second = slots_of(ids_ref[...])
    picks = jnp.where(first | second, 1.0, 0.0).astype(BF16)
    fetch_tokens.wait()
    chosen = jnp.dot(picks, tokens_ref[...], preferred_element_type=F32).astype(BF16)
    keep_ref[...] = chosen[:KEPT]
    send_ref[...] = chosen[KEPT:]


def select(ids, tokens):
    kept = jax.ShapeDtypeStruct((KEPT, tokens.shape[1]), BF16)
    return pl.pallas_call(
        select_kernel,
        out_shape=[kept, kept],
        in_specs=hbm(2),
        out_specs=vmem(2),
        scratch_shapes=[
            pltpu.VMEM(ids.shape, ids.dtype),
            pltpu.VMEM(tokens.shape, BF16),
            pltpu.SemaphoreType.DMA((2,)),
        ],
        compiler_params=pltpu.CompilerParams(vmem_limit_bytes=4 << 20),
        name="select",
    )(*in_hbm(ids, tokens))


def in_blocks(row):
    block = (row * 1639) >> 16
    inside = row - block * BLOCK
    half = jnp.where(inside < CAP, 0, 1)
    return block, inside, half


def shuffle_kernel(keep_ref, came_ref, *out_refs):
    def source_of(row):
        block, inside, half = in_blocks(row)
        return half * KEPT + block * CAP + inside - half * CAP, inside < 2 * CAP

    rows = moved((FAR * BLOCK, 0), source_of, keep_ref, came_ref)
    for k, out in enumerate(out_refs):
        out[...] = rows[k * BLOCK : (k + 1) * BLOCK].astype(BF16)


def pack_kernel(*refs):
    *blocks, sums_ref, out_ref = refs

    def source_of(row):
        block = (row * 1821) >> 16
        return block * BLOCK + row - block * 2 * CAP, row >= 0

    out_ref[:ROWS] = moved((ROWS, 0), source_of, *blocks).astype(BF16)
    out_ref[ROWS:] = sums_ref[...]


def pair_kernel(first_ref, second_ref, out_ref):
    out_ref[0] = first_ref[...]
    out_ref[1] = second_ref[...]


def views(tiles, keys):
    arrays = []
    where = []
    for key in keys:
        array, at = tiles[key]
        known = [n for n, a in enumerate(arrays) if a is array]
        if not known:
            known = [len(arrays)]
            arrays.append(array)
        where.append((known[0], at))
    return arrays, where


def viewed(refs, where):
    return [refs[n] if at is None else refs[n].at[at] for n, at in where]


def unpack_kernel(*refs):
    terms, out_refs = refs[:-FAR], refs[-FAR:]
    total = sum(t[...].astype(F32) for t in terms).astype(BF16)

    def source_of(row):
        block, inside, _ = in_blocks(row)
        return block * 2 * CAP + inside, inside < 2 * CAP

    rows = moved((FAR * BLOCK, 0), source_of, total)
    for k, out in enumerate(out_refs):
        out[...] = rows[k * BLOCK : (k + 1) * BLOCK].astype(BF16)


def unshuffle_kernel(*refs):
    blocks, (keep_ref, send_ref) = refs[:FAR], refs[FAR:]

    def source_of(row):
        k = (row * 3641) >> 16
        return (k & 3) * BLOCK + (k >> 2) * CAP + row - k * CAP, row >= 0

    rows = moved((ROWS, 0), source_of, *blocks).astype(BF16)
    keep_ref[...] = rows[:KEPT]
    send_ref[...] = rows[KEPT:]


def transposed_dot(left, right):
    return lax.dot_general(left, right, (((1,), (1,)), ((), ())), preferred_element_type=F32)


def halves(value):
    high = value.astype(BF16)
    return high, (value - high.astype(F32)).astype(BF16)


def stats_kernel(tokens_hbm, gain_hbm, router_hbm, *refs):
    weights, out_ref, gain_ref, weight_refs = refs[:3], refs[3], refs[4], refs[5:8]
    tokens_ref, router_ref, sems, weight_sems = refs[8:]
    tokens, width = tokens_ref.shape
    part = lax.axis_index("zl") * 4 + lax.axis_index("x")
    here = pl.ds(pl.multiple_of(part * width, width), width)
    ways = ((tokens_hbm, tokens_ref), (gain_hbm, gain_ref), (router_hbm.at[:, here], router_ref))
    fetches = [pltpu.make_async_copy(a, b, sems.at[n]) for n, (a, b) in enumerate(ways)]
    for fetch in fetches:
        fetch.start()
    later = [
        pltpu.make_async_copy(a, b, weight_sems.at[n])
        for n, (a, b) in enumerate(zip(weights, weight_refs))
    ]
    for fetch in later:
        fetch.start()
    out_ref[...] = jnp.zeros_like(out_ref)
    for fetch in fetches:
        fetch.wait()
    values = tokens_ref[...].astype(F32)
    router = router_ref[...]
    ones = jnp.ones_like(router)
    scaled, squares = halves(values * gain_ref[:, here]), halves(values * values)
    for n, (left, terms) in enumerate(((router, scaled), (ones, squares))):
        for k, v in enumerate(halves(sum(transposed_dot(left, t) for t in terms))):
            start = (2 * n + k) * 128
            out_ref[:, start : start + tokens] = v
    for fetch in later:
        fetch.wait()


def stats(tokens, gain, router, *weights):
    width = tokens.shape[1]
    return pl.pallas_call(
        stats_kernel,
        out_shape=[
            jax.ShapeDtypeStruct((EXTRA, width), BF16),
            jax.ShapeDtypeStruct(gain.shape, F32),
            *(jax.ShapeDtypeStruct(w.shape, BF16) for w in weights),
        ],
        in_specs=hbm(6),
        out_specs=vmem(5),
        scratch_shapes=[
            pltpu.VMEM(tokens.shape, BF16),
            pltpu.VMEM((router.shape[0], width), BF16),
            pltpu.SemaphoreType.DMA((3,)),
            pltpu.SemaphoreType.DMA((3,)),
        ],
        compiler_params=pltpu.CompilerParams(vmem_limit_bytes=4 << 20),
        name="stats",
    )(*in_hbm(tokens, gain, router, *weights))


def stats_in(tile, tokens):
    parts = [tile[ROWS:, n * 128 : n * 128 + tokens].astype(F32) for n in range(4)]
    return parts[0] + parts[1], parts[2] + parts[3]


def combine_kernel(width_all, ids_ref, sums_ref, keep_ref, came_ref, out_ref):
    ids = ids_ref[...]
    sums = sums_ref[...]
    experts = sums.shape[0] // 2
    scale = lax.rsqrt(sums[experts : experts + 1] / width_all + EPSILON)
    named = lax.broadcasted_iota(jnp.int32, (experts, ids.shape[1]), 0)
    logits = [
        jnp.sum(jnp.where(named == ids[k : k + 1], sums[:experts], 0.0), axis=0, keepdims=True)
        * scale
        for k in (0, 1)
    ]
    gate_first = 1.0 / (1.0 + jnp.exp(logits[1] - logits[0]))
    gate_second = 1.0 / (1.0 + jnp.exp(logits[0] - logits[1]))
    first, second = slots_of(ids)
    weights = jnp.where(first, gate_first, 0.0) + jnp.where(second, gate_second, 0.0)
    rows = jnp.concatenate([keep_ref[...], came_ref[...]], axis=0)
    out_ref[...] = sum(
        lax.dot_general(w, rows, (((0,), (0,)), ((), ())), preferred_element_type=F32)
        for w in halves(weights)
    ).astype(BF16)


def offset_place(square, ring):
    step = jnp.where(ring == 1, 3, jnp.where(ring == 2, 1, jnp.where(ring == 3, 2, 0)))
    feature = (lax.axis_index("zl") ^ (square >> 1)) * 4 + ((lax.axis_index("x") + step) & 3)
    return square & 1, feature


def tile_place(outer, inner):
    core = lax.axis_index("c")
    return offset_place(jnp.where(core == 0, outer, inner), jnp.where(core == 0, inner, outer))


CHUNK = 48
FIRST = ((0, 0), (0, 1), (0, 2), (0, 3), (1, 0), (1, 3), (2, 1), (2, 2))
SECOND = ((1, 1), (1, 2), (2, 0), (2, 3))
LAST = ((3, 0), (3, 1), (3, 2), (3, 3))


def prepare(tile, gain, out_ref, row_start, column_at, squares_ref, squares_start):
    width = tile.shape[1]

    def step(n, _):
        at = pl.multiple_of(n * CHUNK, CHUNK)
        values = tile[pl.ds(at, CHUNK), :].astype(F32)
        row_at = pl.ds(pl.multiple_of(row_start + at, 16), CHUNK)
        out_ref[row_at, column_at] = (values * gain).astype(BF16)
        square = values * values
        squares_at = pl.ds(pl.multiple_of(squares_start + at, 16), CHUNK)
        squares_ref[squares_at, :] += sum(
            square[:, j * 128 : (j + 1) * 128] for j in range(width // 128)
        )
        return 0

    lax.fori_loop(0, ROWS // CHUNK, step, 0)


def add_stats(tile, row_class, sums_ref):
    experts, tokens = sums_ref.shape[0] // 2, sums_ref.shape[1]
    own = jnp.where(row_class == 0, 1.0, 0.0)
    logits, squares = stats_in(tile, tokens)
    sums_ref[:experts] += logits * own
    sums_ref[experts:] += squares * own


def columns_of(feature, width):
    return pl.ds(pl.multiple_of(feature * width, width), width)


def place_tile(key, tile, gain_ref, x_ref, squares_ref, sums_ref):
    row_class, feature = tile_place(*key)
    column_at = columns_of(feature, tile.shape[1])
    start = row_class * ROWS
    prepare(tile, gain_ref[:, column_at], x_ref, start, column_at, squares_ref, start)
    add_stats(tile, row_class, sums_ref)


def fill_kernel(where, gain_ref, *refs):
    tiles, (x_ref, squares_ref, sums_ref) = viewed(refs, where), refs[-3:]
    width = tiles[0].shape[1]
    squares_ref[...] = jnp.zeros_like(squares_ref)
    sums_ref[...] = jnp.zeros_like(sums_ref)
    for key, tile in zip(FIRST, tiles):
        place_tile(key, tile, gain_ref, x_ref, squares_ref, sums_ref)
    for key in LAST:
        row_class, feature = tile_place(*key)
        row_at = pl.ds(pl.multiple_of(row_class * ROWS, ROWS), ROWS)
        x_ref[row_at, columns_of(feature, width)] = jnp.zeros((ROWS, width), BF16)


def early_kernel(where, gain_ref, *refs):
    tiles, weights = viewed(refs, where), refs[-11:-7]
    acc_ref, x_ref, squares_ref, sums_ref = refs[-4:]
    for key, tile in zip(SECOND, tiles):
        place_tile(key, tile, gain_ref, x_ref, squares_ref, sums_ref)
    for n, weight in enumerate(weights):
        acc_ref[n] = jnp.dot(x_ref[...], weight[...], preferred_element_type=F32)


def early_of(gain, tiles, weights, sums_shape):
    width_all, slices = weights[0].shape
    given = [
        jax.ShapeDtypeStruct((2 * ROWS, width_all), BF16),
        jax.ShapeDtypeStruct((2 * ROWS, 128), F32),
        jax.ShapeDtypeStruct(sums_shape, F32),
    ]
    arrays, where = views(tiles, FIRST)
    filled = pl.pallas_call(
        partial(fill_kernel, where),
        out_shape=given,
        in_specs=vmem(1 + len(arrays)),
        out_specs=vmem(3),
        compiler_params=pltpu.CompilerParams(vmem_limit_bytes=8 << 20),
        name="fill",
    )(gain, *arrays)
    arrays, where = views(tiles, SECOND)
    at = 1 + len(arrays) + 4
    acc, _, squares, sums = pl.pallas_call(
        partial(early_kernel, where),
        out_shape=[jax.ShapeDtypeStruct((4, 2 * ROWS, slices), F32), *given],
        in_specs=vmem(at + 3),
        out_specs=vmem(4),
        input_output_aliases={at + n: 1 + n for n in range(3)},
        compiler_params=pltpu.CompilerParams(vmem_limit_bytes=12 << 20),
        cost_estimate=pl.CostEstimate(
            flops=2 * 2 * ROWS * width_all * 4 * slices,
            bytes_accessed=4 * width_all * slices * 2,
            transcendentals=0,
        ),
        name="early",
    )(gain, *arrays, *weights, *filled)
    return acc, squares, sums


def late_kernel(width_all, where, gain_ref, *refs):
    tiles, weights = viewed(refs, where), refs[-12:-8]
    _, squares_in, sums_in, out_ref, sums_ref, acc_ref, squares_ref, x_ref = refs[-8:]
    width = tiles[0].shape[1]
    slices = weights[0].shape[1]
    squares_ref[...] = squares_in[...]
    sums_ref[...] = sums_in[...]
    for key, tile in zip(LAST, tiles):
        row_class, feature = tile_place(*key)
        column_at = columns_of(feature, width)
        start = row_class * ROWS
        gain = gain_ref[:, column_at]
        prepare(tile, gain, x_ref, 0, slice(None), squares_ref, start)
        add_stats(tile, row_class, sums_ref)
        row_at = pl.ds(pl.multiple_of(start, ROWS), ROWS)
        for n, weight in enumerate(weights):
            acc_ref[n, row_at, :] = acc_ref[n, row_at, :] + jnp.dot(
                x_ref[...], weight[column_at, :], preferred_element_type=F32
            )
    scale = lax.rsqrt(jnp.sum(squares_ref[...], axis=1, keepdims=True) / width_all + EPSILON)
    for half in range(2):
        gate, up = acc_ref[2 * half] * scale, acc_ref[2 * half + 1] * scale
        start = (1 - half) * slices
        out_ref[:, start : start + slices] = (gate * (1.0 / (1.0 + jnp.exp(-gate))) * up).astype(
            BF16
        )


def late_of(gain, tiles, weights, acc, squares, sums):
    width_all, slices = weights[0].shape
    arrays, where = views(tiles, LAST)
    width = arrays[0].shape[-1]
    at = 1 + len(arrays) + 4
    return pl.pallas_call(
        partial(late_kernel, width_all, where),
        out_shape=[
            jax.ShapeDtypeStruct((2 * ROWS, 2 * slices), BF16),
            jax.ShapeDtypeStruct(sums.shape, F32),
            jax.ShapeDtypeStruct(acc.shape, F32),
        ],
        in_specs=vmem(at + 3),
        out_specs=vmem(3),
        input_output_aliases={at: 2},
        scratch_shapes=[
            pltpu.VMEM(squares.shape, F32),
            pltpu.VMEM((ROWS, width), BF16),
        ],
        compiler_params=pltpu.CompilerParams(vmem_limit_bytes=12 << 20),
        cost_estimate=pl.CostEstimate(
            flops=2 * 4 * ROWS * width * 4 * slices,
            bytes_accessed=acc.size * 8,
            transcendentals=0,
        ),
        name="late",
    )(gain, *arrays, *weights, acc, squares, sums)[:2]


def down_kernel(far, places, hidden_ref, own_ref, other_ref, *refs):
    out_refs, y_ref = refs[:-1], refs[-1]
    slices = own_ref.shape[0]
    width = y_ref.shape[2]
    core = lax.axis_index("c")

    def product(rows, square, ring):
        _, feature = offset_place(square, ring)
        column_at = columns_of(feature, width)
        return (
            jnp.dot(hidden_ref[rows, :slices], own_ref[:, column_at], preferred_element_type=F32)
            + jnp.dot(hidden_ref[rows, slices:], other_ref[:, column_at], preferred_element_type=F32)
        ).astype(BF16)

    both, first, last = slice(None), slice(0, ROWS), slice(ROWS, 2 * ROWS)

    @pl.when(core == 0)
    def _():
        def step(ring, _):
            if far:
                y_ref[ring] = product(last, 3, ring)
                return 0
            pair = product(both, 0, ring)
            y_ref[ring] = pair[:ROWS]
            y_ref[4 + ring] = pair[ROWS:]
            y_ref[8 + ring] = product(first, 2, ring)
            return 0

        lax.fori_loop(0, 4, step, 0)

    @pl.when(core == 1)
    def _():
        def step(n, _):
            ring, square = (3, 2 * n) if far else (n >> 1, 2 * (n & 1))
            pair = product(both, square, ring)
            at = square if far else 4 * ring + square
            y_ref[at] = pair[:ROWS]
            y_ref[at + 1] = pair[ROWS:]
            return 0

        lax.fori_loop(0, 2 if far else 6, step, 0)

    for index, (at, start) in enumerate(places):
        out_refs[at][start : start + ROWS, :] = y_ref[index]


def down_of(far, shapes, places, hidden, own, other):
    slices, width_all = own.shape
    width = width_all // 8
    return pl.pallas_call(
        partial(down_kernel, far, places),
        out_shape=[jax.ShapeDtypeStruct((rows, width), BF16) for rows in shapes],
        in_specs=vmem(3),
        out_specs=vmem(len(shapes)),
        scratch_shapes=[pltpu.VMEM((len(places), ROWS, width), BF16)],
        compiler_params=pltpu.CompilerParams(vmem_limit_bytes=16 << 20),
        cost_estimate=pl.CostEstimate(
            flops=2 * len(places) * ROWS * width * 2 * slices,
            bytes_accessed=2 * slices * width_all * 2,
            transcendentals=0,
        ),
        name="far" if far else "rest",
    )(hidden, own, other)


def added_kernel(starts, *refs):
    *terms, out_ref = refs
    rows = out_ref.shape[0]
    out_ref[...] = sum(t[n : n + rows, :].astype(F32) for t, n in zip(terms, starts)).astype(BF16)


def added(*terms):
    terms = [t if isinstance(t, tuple) else (t, 0) for t in terms]
    (out,) = small(
        partial(added_kernel, [n for _, n in terms]),
        [(ROWS, terms[0][0].shape[1])],
        *(t for t, _ in terms),
    )
    return out


def per_device(tokens, norm_gain, router_weight, expert_ids, gate_proj, up_proj, down_proj):
    width_all = router_weight.shape[0]
    width = tokens.shape[1]
    gain = norm_gain.reshape(1, width_all)
    ids = expert_ids.T
    kept, block = (KEPT, width), (BLOCK, width)

    keep, send = select(ids, tokens)
    came = across_y(send)
    blocks = small(shuffle_kernel, [block] * FAR, keep, came)
    arrived = [blocks[0]] + [along_z(blocks[k], k) for k in (1, 2, 3)]
    gate_other = other_core(gate_proj)
    up_other = other_core(up_proj)
    down_other = other_core(down_proj)
    part_sums, gain, gate_own, up_own, down_own = stats(
        tokens, gain, router_weight.T, gate_proj, up_proj, down_proj
    )
    (mine,) = small(pack_kernel, [(ROWS + EXTRA, width)], *arrived, part_sums)

    one = hop(mine, "x+", "y")
    two = hop(mine, "x-", "z")
    opposite = hop(mine, "xx", "yz")
    (pair,) = small(pair_kernel, [(2, ROWS + EXTRA, width)], one, two)
    ring_one = [hop(v, "y", "x+") for v in (mine, pair, opposite)]
    ring_two = [hop(v, "z", "x-") for v in (mine, pair, opposite)]
    far_ones = [
        hop(ring_one[0], "z", "x+"), hop(ring_two[1], "y", "x-"), hop(ring_one[2], "z", "x+")
    ]
    tiles = {(0, 0): (mine, None), (0, 1): (one, None), (0, 2): (two, None), (0, 3): (opposite, None)}
    for m, ring in enumerate((ring_one, ring_two, far_ones), 1):
        tiles[m, 0], tiles[m, 3] = (ring[0], None), (ring[2], None)
        tiles[m, 1], tiles[m, 2] = (ring[1], 0), (ring[1], 1)

    sums_shape = (2 * router_weight.shape[1], tokens.shape[0])
    weights = (gate_other, up_other, gate_own, up_own)
    acc, squares, sums = early_of(gain, tiles, weights, sums_shape)
    hidden, sums = late_of(gain, tiles, weights, acc, squares, sums)

    places = [(0, 0), (0, ROWS), (1, 0), (1, ROWS)]
    far = down_of(True, [2 * ROWS] * 2, places, hidden, down_own, down_other)
    places = [(a, 0) for a in range(4)]
    places += [(4, 0), (5, 0), (8, 0), (8, ROWS)]
    places += [(9, 0), (10, 0), (6, 0), (7, 0)]
    shapes = [ROWS] * 8 + [2 * ROWS] + [ROWS] * 2
    rest = down_of(False, shapes, places, hidden, down_own, down_other)
    own, near, pair, singles = rest[:4], rest[4:8], rest[8], rest[9:]
    far_pairs = [hop(far[0], "z", "x-"), hop(far[1], "y", "x+")]
    far_in = [(far_pairs[n >> 1], (n & 1) * ROWS) for n in range(4)]
    pair_in = hop(pair, "y", "x-")
    singles_in = [hop(singles[n], "z", "x+") for n in range(2)]
    ways = [("y", "x-"), ("y", "x-"), ("z", "x+"), ("z", "x+")]
    near_in = [hop(added(near[n], far_in[n]), *ways[n]) for n in range(4)]
    parts = [
        (own[0], near_in[0], singles_in[0]),
        (own[1], near_in[1], singles_in[1]),
        (own[2], near_in[2], (pair_in, 0)),
        (own[3], near_in[3], (pair_in, ROWS)),
    ]
    terms = [
        *parts[0],
        hop(added(*parts[1]), "x-", "y"),
        hop(added(*parts[2]), "x+", "z"),
        hop(added(*parts[3]), "xx", "yz"),
    ]
    blocks = small(unpack_kernel, [block] * FAR, *terms)
    back = [blocks[0]] + [along_z(blocks[k], FAR - k) for k in (1, 2, 3)]
    keep, send = small(unshuffle_kernel, [kept, kept], *back)
    came = across_y(send)
    return pl.pallas_call(
        partial(combine_kernel, width_all),
        out_shape=jax.ShapeDtypeStruct(tokens.shape, BF16),
        in_specs=vmem(4),
        out_specs=vmem(1)[0],
        compiler_params=pltpu.CompilerParams(vmem_limit_bytes=4 << 20),
        name="combine",
    )(ids, sums, keep, came)


def solution(mesh):
    cut = Mesh(mesh.devices.reshape(SIZES), AXES)
    split = GRP + TP
    placed = (
        P(GRP, TP),
        P(),
        P(),
        P(GRP, None),
        P(None, split),
        P(None, split),
        P(split, None),
    )

    return jax.shard_map(per_device, mesh=cut, in_specs=placed, out_specs=P(GRP, TP), check_vma=False)
```

```python
from functools import partial

import jax
import jax.numpy as jnp
from jax import lax
from jax.experimental import pallas as pl
from jax.experimental.pallas import tpu as pltpu
from jax.sharding import Mesh
from jax.sharding import PartitionSpec as P


AXES = ("zh", "y2", "y1", "c", "zl", "x")
SIZES = (4, 2, 2, 2, 2, 4)
GRP = ("zh", "y2", "y1", "c")
TP = ("zl", "x")
OWNER = ("y1", "c", "zl", "x")
CAP = 18
FAR = 4
KEPT = FAR * CAP
ROWS = 2 * KEPT
NEAR = 56
CROSSED = 24
EXTRA = 8
BLOCK = 40
EPSILON = 1e-05
F32 = jnp.float32
BF16 = jnp.bfloat16


def place(y, z, x, step):
    if step == "x+":
        return y, z, (x + 1) % 4
    if step == "x-":
        return y, z, (x - 1) % 4
    if step == "xx":
        return y, z, (x + 2) % 4
    if step == "y":
        return 1 - y, z, x
    if step == "z":
        return y, 1 - z, x
    return 1 - y, 1 - z, x


def owner_pairs(*steps):
    pairs = []
    for y in range(2):
        for z in range(2):
            for x in range(4):
                for group, step in enumerate(steps):
                    ends = ((y, z, x), place(y, z, x, step))
                    pairs.append(
                        tuple(((j * 2 + (group ^ (j + k + n) & 1)) * 2 + k) * 4 + n for j, k, n in ends)
                    )
    return pairs


def hop(value, step_core0, step_core1):
    return lax.ppermute(value, OWNER, owner_pairs(step_core0, step_core1))


def along_z(value, distance):
    pairs = []
    for h in range(FAR):
        for c in range(2):
            for z in range(2):
                for x in range(4):
                    target = (h + distance) % FAR, c ^ (z + x) & 1
                    pairs.append(
                        tuple(((i * 2 + j) * 2 + z) * 4 + x for i, j in ((h, c), target))
                    )
    return lax.ppermute(value, ("zh", "c", "zl", "x"), pairs)


def across_y(value):
    pairs = [(i * 2 + c, (3 - i) * 2 + 1 - c) for i in range(4) for c in range(2)]
    return lax.ppermute(value, ("y2", "y1", "c"), pairs)


def other_core(value):
    return lax.ppermute(value, "c", [(0, 1), (1, 0)])


def vmem(count):
    return [pl.BlockSpec(memory_space=pltpu.VMEM)] * count


def hbm(count):
    return [pl.BlockSpec(memory_space=pltpu.HBM)] * count


def in_hbm(*arrays):
    return [pltpu.with_memory_space_constraint(a, pltpu.HBM) for a in arrays]


def small(kernel, outs, *operands):
    return pl.pallas_call(
        kernel,
        out_shape=[jax.ShapeDtypeStruct(shape, BF16) for shape in outs],
        in_specs=vmem(len(operands)),
        out_specs=vmem(len(outs)),
        compiler_params=pltpu.CompilerParams(vmem_limit_bytes=4 << 20),
    )(*operands)


def moved(shape, source_of, *blocks):
    joined = jnp.concatenate([b[...] for b in blocks], axis=0)
    row = lax.broadcasted_iota(jnp.int32, (shape[0], joined.shape[0]), 0)
    column = lax.broadcasted_iota(jnp.int32, (shape[0], joined.shape[0]), 1)
    source, valid = source_of(row)
    picks = jnp.where((source == column) & valid, 1.0, 0.0).astype(BF16)
    return jnp.dot(picks, joined, preferred_element_type=F32)


def leaving(row):
    part = jnp.where(row >= NEAR, 1, 0) + jnp.where(row >= 2 * NEAR, 1, 0)
    row = row - part * NEAR
    k = (row * 3641) >> 16
    half = jnp.where(part == 2, k, part)
    distance = jnp.where(part == 2, 2, jnp.where(k == 2, 3, k))
    return half, distance, row - k * CAP, k < jnp.where(part == 2, 2, 3)


def returning(row):
    k = (row * 3641) >> 16
    return k >> 2, k & 3, row - k * CAP, row >= 0


def slots_of(ids, order, rows):
    tokens = ids.shape[1]
    slot = lax.broadcasted_iota(jnp.int32, (rows, tokens), 0)
    half, distance, inside, valid = order(slot)
    zh, y2 = lax.axis_index("zh"), lax.axis_index("y2")
    expert = ((zh + distance) & 3) * 2 + (y2 ^ half)
    first, second = ids[0:1, :] == expert, ids[1:2, :] == expert
    routed = jnp.where(first | second, 1.0, 0.0).astype(BF16)
    earlier = lax.broadcasted_iota(jnp.int32, (tokens, tokens), 0) < lax.broadcasted_iota(
        jnp.int32, (tokens, tokens), 1
    )
    before = jnp.dot(
        routed, jnp.where(earlier, 1.0, 0.0).astype(BF16), preferred_element_type=F32
    )
    here = (before == inside.astype(F32)) & valid
    return first & here, second & here


def select_kernel(ids_hbm, tokens_hbm, keep_ref, send_ref, far_ref, ids_ref, tokens_ref, sems):
    fetch = pltpu.make_async_copy(ids_hbm, ids_ref, sems.at[0])
    fetch_tokens = pltpu.make_async_copy(tokens_hbm, tokens_ref, sems.at[1])
    fetch.start()
    fetch_tokens.start()
    fetch.wait()
    first, second = slots_of(ids_ref[...], leaving, 2 * NEAR + BLOCK)
    picks = jnp.where(first | second, 1.0, 0.0).astype(BF16)
    fetch_tokens.wait()
    chosen = jnp.dot(picks, tokens_ref[...], preferred_element_type=F32).astype(BF16)
    keep_ref[...] = chosen[:NEAR]
    send_ref[...] = chosen[NEAR : 2 * NEAR]
    far_ref[...] = chosen[2 * NEAR :]


def select(ids, tokens):
    sizes = (NEAR, NEAR, BLOCK)
    return pl.pallas_call(
        select_kernel,
        out_shape=[jax.ShapeDtypeStruct((n, tokens.shape[1]), BF16) for n in sizes],
        in_specs=hbm(2),
        out_specs=vmem(3),
        scratch_shapes=[
            pltpu.VMEM(ids.shape, ids.dtype),
            pltpu.VMEM(tokens.shape, BF16),
            pltpu.SemaphoreType.DMA((2,)),
        ],
        compiler_params=pltpu.CompilerParams(vmem_limit_bytes=4 << 20),
        name="select",
    )(*in_hbm(ids, tokens))


def in_blocks(row):
    block = (row * 1639) >> 16
    inside = row - block * BLOCK
    half = jnp.where(inside < CAP, 0, 1)
    return block, inside, half


def shuffle_kernel(keep_ref, came_ref, sums_ref, stay_ref, *out_refs):
    def source_of(row):
        block, inside, half = in_blocks(row)
        return half * NEAR + block * CAP + inside - half * CAP, inside < 2 * CAP

    rows = moved((3 * BLOCK, 0), source_of, keep_ref, came_ref)
    stay_ref[:BLOCK] = rows[:BLOCK].astype(BF16)
    stay_ref[BLOCK:] = sums_ref[...]
    for k, out in enumerate(out_refs, 1):
        out[...] = rows[k * BLOCK : (k + 1) * BLOCK].astype(BF16)


def cross_kernel(far_ref, out_ref):
    def source_of(row):
        return row + CAP, row < CAP

    out_ref[...] = moved((CROSSED, 0), source_of, far_ref).astype(BF16)


def pack_kernel(stay_ref, one_ref, two_ref, three_ref, crossed_ref, out_ref):
    start = BLOCK + EXTRA

    def source_of(row):
        block = (row * 1821) >> 16
        inside = row - block * 2 * CAP
        source = jnp.where(block == 0, 0, start + (block - 1) * BLOCK) + inside
        crossed = (block == 2) & (inside >= CAP)
        return jnp.where(crossed, start + 3 * BLOCK + inside - CAP, source), row >= 0

    refs = (stay_ref, one_ref, two_ref, three_ref, crossed_ref)
    out_ref[:ROWS] = moved((ROWS, 0), source_of, *refs).astype(BF16)
    out_ref[ROWS:] = stay_ref[BLOCK:]


def pair_kernel(first_ref, second_ref, out_ref):
    out_ref[0] = first_ref[...]
    out_ref[1] = second_ref[...]


def views(tiles, keys):
    arrays = []
    where = []
    for key in keys:
        array, at = tiles[key]
        known = [n for n, a in enumerate(arrays) if a is array]
        if not known:
            known = [len(arrays)]
            arrays.append(array)
        where.append((known[0], at))
    return arrays, where


def viewed(refs, where):
    return [refs[n] if at is None else refs[n].at[at] for n, at in where]


def unpack_kernel(*refs):
    terms, out_refs = refs[:-FAR], refs[-FAR:]
    total = sum(t[...].astype(F32) for t in terms).astype(BF16)

    def source_of(row):
        block, inside, _ = in_blocks(row)
        return block * 2 * CAP + inside, inside < 2 * CAP

    rows = moved((FAR * BLOCK, 0), source_of, total)
    for k, out in enumerate(out_refs):
        out[...] = rows[k * BLOCK : (k + 1) * BLOCK].astype(BF16)


def unshuffle_kernel(*refs):
    blocks, (keep_ref, send_ref) = refs[:FAR], refs[FAR:]

    def source_of(row):
        k = (row * 3641) >> 16
        return (k & 3) * BLOCK + (k >> 2) * CAP + row - k * CAP, row >= 0

    rows = moved((ROWS, 0), source_of, *blocks).astype(BF16)
    keep_ref[...] = rows[:KEPT]
    send_ref[...] = rows[KEPT:]


def transposed_dot(left, right):
    return lax.dot_general(left, right, (((1,), (1,)), ((), ())), preferred_element_type=F32)


def halves(value):
    high = value.astype(BF16)
    return high, (value - high.astype(F32)).astype(BF16)


def stats_kernel(tokens_hbm, gain_hbm, router_hbm, out_ref, gain_ref, tokens_ref, router_ref, sems):
    tokens, width = tokens_ref.shape
    part = lax.axis_index("zl") * 4 + lax.axis_index("x")
    here = pl.ds(pl.multiple_of(part * width, width), width)
    ways = ((tokens_hbm, tokens_ref), (gain_hbm, gain_ref), (router_hbm.at[:, here], router_ref))
    fetches = [pltpu.make_async_copy(a, b, sems.at[n]) for n, (a, b) in enumerate(ways)]
    for fetch in fetches:
        fetch.start()
    out_ref[...] = jnp.zeros_like(out_ref)
    for fetch in fetches:
        fetch.wait()
    values = tokens_ref[...].astype(F32)
    router = router_ref[...]
    ones = jnp.ones_like(router)
    scaled, squares = halves(values * gain_ref[:, here]), halves(values * values)
    for n, (left, terms) in enumerate(((router, scaled), (ones, squares))):
        for k, v in enumerate(halves(sum(transposed_dot(left, t) for t in terms))):
            start = (2 * n + k) * 128
            out_ref[:, start : start + tokens] = v


def stats(tokens, gain, router):
    width = tokens.shape[1]
    return pl.pallas_call(
        stats_kernel,
        out_shape=[
            jax.ShapeDtypeStruct((EXTRA, width), BF16),
            jax.ShapeDtypeStruct(gain.shape, F32),
        ],
        in_specs=hbm(3),
        out_specs=vmem(2),
        scratch_shapes=[
            pltpu.VMEM(tokens.shape, BF16),
            pltpu.VMEM((router.shape[0], width), BF16),
            pltpu.SemaphoreType.DMA((3,)),
        ],
        compiler_params=pltpu.CompilerParams(vmem_limit_bytes=4 << 20),
        name="stats",
    )(*in_hbm(tokens, gain, router))


def fetch_kernel(*refs):
    count = len(refs) // 2
    sems = refs[-1]
    copies = [
        pltpu.make_async_copy(refs[n], refs[count + n], sems.at[n]) for n in range(count)
    ]
    for copy in copies:
        copy.start()
    for copy in copies:
        copy.wait()


def fetched(*arrays):
    return pl.pallas_call(
        fetch_kernel,
        out_shape=[jax.ShapeDtypeStruct(a.shape, a.dtype) for a in arrays],
        in_specs=hbm(len(arrays)),
        out_specs=vmem(len(arrays)),
        scratch_shapes=[pltpu.SemaphoreType.DMA((len(arrays),))],
        compiler_params=pltpu.CompilerParams(vmem_limit_bytes=4 << 20),
        name="fetch",
    )(*in_hbm(*arrays))


def stats_in(tile, tokens):
    parts = [tile[ROWS:, n * 128 : n * 128 + tokens].astype(F32) for n in range(4)]
    return parts[0] + parts[1], parts[2] + parts[3]


def combine_kernel(width_all, ids_ref, sums_ref, keep_ref, came_ref, out_ref):
    ids = ids_ref[...]
    sums = sums_ref[...]
    experts = sums.shape[0] // 2
    scale = lax.rsqrt(sums[experts : experts + 1] / width_all + EPSILON)
    named = lax.broadcasted_iota(jnp.int32, (experts, ids.shape[1]), 0)
    logits = [
        jnp.sum(jnp.where(named == ids[k : k + 1], sums[:experts], 0.0), axis=0, keepdims=True)
        * scale
        for k in (0, 1)
    ]
    gate_first = 1.0 / (1.0 + jnp.exp(logits[1] - logits[0]))
    gate_second = 1.0 / (1.0 + jnp.exp(logits[0] - logits[1]))
    first, second = slots_of(ids, returning, ROWS)
    weights = jnp.where(first, gate_first, 0.0) + jnp.where(second, gate_second, 0.0)
    rows = jnp.concatenate([keep_ref[...], came_ref[...]], axis=0)
    out_ref[...] = sum(
        lax.dot_general(w, rows, (((0,), (0,)), ((), ())), preferred_element_type=F32)
        for w in halves(weights)
    ).astype(BF16)


def offset_place(square, ring):
    step = jnp.where(ring == 1, 3, jnp.where(ring == 2, 1, jnp.where(ring == 3, 2, 0)))
    feature = (lax.axis_index("zl") ^ (square >> 1)) * 4 + ((lax.axis_index("x") + step) & 3)
    return square & 1, feature


def group_index():
    place_sum = lax.axis_index("y1") + lax.axis_index("zl") + lax.axis_index("x")
    return lax.axis_index("c") ^ (place_sum & 1)


def tile_place(outer, inner):
    group = group_index()
    return offset_place(jnp.where(group == 0, outer, inner), jnp.where(group == 0, inner, outer))


CHUNK = 48
FIRST = ((0, 0), (0, 1), (0, 2), (0, 3), (1, 0), (1, 3), (2, 1), (2, 2))
SECOND = ((1, 1), (1, 2), (2, 0), (2, 3))
LAST = ((3, 0), (3, 1), (3, 2), (3, 3))


def prepare(tile, gain, out_ref, row_start, column_at, squares_ref, squares_start):
    width = tile.shape[1]

    def step(n, _):
        at = pl.multiple_of(n * CHUNK, CHUNK)
        values = tile[pl.ds(at, CHUNK), :].astype(F32)
        row_at = pl.ds(pl.multiple_of(row_start + at, 16), CHUNK)
        out_ref[row_at, column_at] = (values * gain).astype(BF16)
        square = values * values
        squares_at = pl.ds(pl.multiple_of(squares_start + at, 16), CHUNK)
        squares_ref[squares_at, :] += sum(
            square[:, j * 128 : (j + 1) * 128] for j in range(width // 128)
        )
        return 0

    lax.fori_loop(0, ROWS // CHUNK, step, 0)


def add_stats(tile, row_class, sums_ref):
    experts, tokens = sums_ref.shape[0] // 2, sums_ref.shape[1]
    own = jnp.where(row_class == 0, 1.0, 0.0)
    logits, squares = stats_in(tile, tokens)
    sums_ref[:experts] += logits * own
    sums_ref[experts:] += squares * own


def columns_of(feature, width):
    return pl.ds(pl.multiple_of(feature * width, width), width)


def place_tile(key, tile, gain_ref, x_ref, squares_ref, sums_ref):
    row_class, feature = tile_place(*key)
    column_at = columns_of(feature, tile.shape[1])
    start = row_class * ROWS
    prepare(tile, gain_ref[:, column_at], x_ref, start, column_at, squares_ref, start)
    add_stats(tile, row_class, sums_ref)


def fill_kernel(where, gain_ref, *refs):
    tiles, (x_ref, squares_ref, sums_ref) = viewed(refs, where), refs[-3:]
    width = tiles[0].shape[1]
    squares_ref[...] = jnp.zeros_like(squares_ref)
    sums_ref[...] = jnp.zeros_like(sums_ref)
    for key, tile in zip(FIRST, tiles):
        place_tile(key, tile, gain_ref, x_ref, squares_ref, sums_ref)
    for key in LAST:
        row_class, feature = tile_place(*key)
        row_at = pl.ds(pl.multiple_of(row_class * ROWS, ROWS), ROWS)
        x_ref[row_at, columns_of(feature, width)] = jnp.zeros((ROWS, width), BF16)


def early_kernel(where, gain_ref, *refs):
    tiles, weights, later = viewed(refs, where), refs[-14:-10], refs[-10]
    later_ref, acc_ref, x_ref, squares_ref, sums_ref, sem = refs[-6:]
    fetch = pltpu.make_async_copy(later, later_ref, sem.at[0])
    fetch.start()
    for key, tile in zip(SECOND, tiles):
        place_tile(key, tile, gain_ref, x_ref, squares_ref, sums_ref)
    for n, weight in enumerate(weights):
        acc_ref[n] = jnp.dot(x_ref[...], weight[...], preferred_element_type=F32)
    fetch.wait()


def early_of(gain, tiles, weights, later, sums_shape):
    width_all, slices = weights[0].shape
    given = [
        jax.ShapeDtypeStruct((2 * ROWS, width_all), BF16),
        jax.ShapeDtypeStruct((2 * ROWS, 128), F32),
        jax.ShapeDtypeStruct(sums_shape, F32),
    ]
    arrays, where = views(tiles, FIRST)
    filled = pl.pallas_call(
        partial(fill_kernel, where),
        out_shape=given,
        in_specs=vmem(1 + len(arrays)),
        out_specs=vmem(3),
        compiler_params=pltpu.CompilerParams(vmem_limit_bytes=8 << 20),
        name="fill",
    )(gain, *arrays)
    arrays, where = views(tiles, SECOND)
    at = 1 + len(arrays) + 5
    later_out, acc, _, squares, sums = pl.pallas_call(
        partial(early_kernel, where),
        out_shape=[
            jax.ShapeDtypeStruct(later.shape, later.dtype),
            jax.ShapeDtypeStruct((4, 2 * ROWS, slices), F32),
            *given,
        ],
        in_specs=vmem(at - 1) + hbm(1) + vmem(3),
        out_specs=vmem(5),
        input_output_aliases={at + n: 2 + n for n in range(3)},
        scratch_shapes=[pltpu.SemaphoreType.DMA((1,))],
        compiler_params=pltpu.CompilerParams(vmem_limit_bytes=12 << 20),
        cost_estimate=pl.CostEstimate(
            flops=2 * 2 * ROWS * width_all * 4 * slices,
            bytes_accessed=4 * width_all * slices * 2,
            transcendentals=0,
        ),
        name="early",
    )(gain, *arrays, *weights, *in_hbm(later), *filled)
    return acc, squares, sums, later_out


def late_kernel(width_all, where, gain_ref, *refs):
    tiles, weights = viewed(refs, where), refs[-12:-8]
    _, squares_in, sums_in, out_ref, sums_ref, acc_ref, squares_ref, x_ref = refs[-8:]
    width = tiles[0].shape[1]
    slices = weights[0].shape[1]
    squares_ref[...] = squares_in[...]
    sums_ref[...] = sums_in[...]
    for key, tile in zip(LAST, tiles):
        row_class, feature = tile_place(*key)
        column_at = columns_of(feature, width)
        start = row_class * ROWS
        gain = gain_ref[:, column_at]
        prepare(tile, gain, x_ref, 0, slice(None), squares_ref, start)
        add_stats(tile, row_class, sums_ref)
        row_at = pl.ds(pl.multiple_of(start, ROWS), ROWS)
        for n, weight in enumerate(weights):
            acc_ref[n, row_at, :] = acc_ref[n, row_at, :] + jnp.dot(
                x_ref[...], weight[column_at, :], preferred_element_type=F32
            )
    scale = lax.rsqrt(jnp.sum(squares_ref[...], axis=1, keepdims=True) / width_all + EPSILON)
    for half in range(2):
        gate, up = acc_ref[2 * half] * scale, acc_ref[2 * half + 1] * scale
        start = (1 - half) * slices
        out_ref[:, start : start + slices] = (gate * (1.0 / (1.0 + jnp.exp(-gate))) * up).astype(
            BF16
        )


def late_of(gain, tiles, weights, acc, squares, sums):
    width_all, slices = weights[0].shape
    arrays, where = views(tiles, LAST)
    width = arrays[0].shape[-1]
    at = 1 + len(arrays) + 4
    return pl.pallas_call(
        partial(late_kernel, width_all, where),
        out_shape=[
            jax.ShapeDtypeStruct((2 * ROWS, 2 * slices), BF16),
            jax.ShapeDtypeStruct(sums.shape, F32),
            jax.ShapeDtypeStruct(acc.shape, F32),
        ],
        in_specs=vmem(at + 3),
        out_specs=vmem(3),
        input_output_aliases={at: 2},
        scratch_shapes=[
            pltpu.VMEM(squares.shape, F32),
            pltpu.VMEM((ROWS, width), BF16),
        ],
        compiler_params=pltpu.CompilerParams(vmem_limit_bytes=12 << 20),
        cost_estimate=pl.CostEstimate(
            flops=2 * 4 * ROWS * width * 4 * slices,
            bytes_accessed=acc.size * 8,
            transcendentals=0,
        ),
        name="late",
    )(gain, *arrays, *weights, acc, squares, sums)[:2]


def down_kernel(far, places, hidden_ref, own_ref, other_ref, *refs):
    out_refs, y_ref = refs[:-1], refs[-1]
    slices = own_ref.shape[0]
    width = y_ref.shape[2]
    group = group_index()

    def product(rows, square, ring):
        _, feature = offset_place(square, ring)
        column_at = columns_of(feature, width)
        return (
            jnp.dot(hidden_ref[rows, :slices], own_ref[:, column_at], preferred_element_type=F32)
            + jnp.dot(hidden_ref[rows, slices:], other_ref[:, column_at], preferred_element_type=F32)
        ).astype(BF16)

    both, first, last = slice(None), slice(0, ROWS), slice(ROWS, 2 * ROWS)

    @pl.when(group == 0)
    def _():
        def step(ring, _):
            if far:
                y_ref[ring] = product(last, 3, ring)
                return 0
            pair = product(both, 0, ring)
            y_ref[ring] = pair[:ROWS]
            y_ref[4 + ring] = pair[ROWS:]
            y_ref[8 + ring] = product(first, 2, ring)
            return 0

        lax.fori_loop(0, 4, step, 0)

    @pl.when(group == 1)
    def _():
        def step(n, _):
            ring, square = (3, 2 * n) if far else (n >> 1, 2 * (n & 1))
            pair = product(both, square, ring)
            at = square if far else 4 * ring + square
            y_ref[at] = pair[:ROWS]
            y_ref[at + 1] = pair[ROWS:]
            return 0

        lax.fori_loop(0, 2 if far else 6, step, 0)

    for index, (at, start) in enumerate(places):
        out_refs[at][start : start + ROWS, :] = y_ref[index]


def down_of(far, shapes, places, hidden, own, other):
    slices, width_all = own.shape
    width = width_all // 8
    return pl.pallas_call(
        partial(down_kernel, far, places),
        out_shape=[jax.ShapeDtypeStruct((rows, width), BF16) for rows in shapes],
        in_specs=vmem(3),
        out_specs=vmem(len(shapes)),
        scratch_shapes=[pltpu.VMEM((len(places), ROWS, width), BF16)],
        compiler_params=pltpu.CompilerParams(vmem_limit_bytes=16 << 20),
        cost_estimate=pl.CostEstimate(
            flops=2 * len(places) * ROWS * width * 2 * slices,
            bytes_accessed=2 * slices * width_all * 2,
            transcendentals=0,
        ),
        name="far" if far else "rest",
    )(hidden, own, other)


def added_kernel(starts, *refs):
    *terms, out_ref = refs
    rows = out_ref.shape[0]
    out_ref[...] = sum(t[n : n + rows, :].astype(F32) for t, n in zip(terms, starts)).astype(BF16)


def added(*terms):
    terms = [t if isinstance(t, tuple) else (t, 0) for t in terms]
    (out,) = small(
        partial(added_kernel, [n for _, n in terms]),
        [(ROWS, terms[0][0].shape[1])],
        *(t for t, _ in terms),
    )
    return out


def per_device(tokens, norm_gain, router_weight, expert_ids, gate_proj, up_proj, down_proj):
    width_all = router_weight.shape[0]
    width = tokens.shape[1]
    gain = norm_gain.reshape(1, width_all)
    ids = expert_ids.T
    kept, block = (KEPT, width), (BLOCK, width)

    keep, send, far = select(ids, tokens)
    part_sums, gain = stats(tokens, gain, router_weight.T)
    came = across_y(send)
    far = along_z(far, 2)
    stay, *blocks = small(
        shuffle_kernel, [(BLOCK + EXTRA, width), block, block], keep, came, part_sums
    )
    one, three = along_z(blocks[0], 1), along_z(blocks[1], 3)
    stay = along_z(stay, 0)
    (crossed,) = small(cross_kernel, [(CROSSED, width)], far)
    crossed = across_y(crossed)
    gate_other = other_core(gate_proj)
    up_other = other_core(up_proj)
    down_other = other_core(down_proj)
    (mine,) = small(pack_kernel, [(ROWS + EXTRA, width)], stay, one, far, three, crossed)
    gate_own, up_own = fetched(gate_proj, up_proj)

    one = hop(mine, "x+", "y")
    two = hop(mine, "x-", "z")
    opposite = hop(mine, "xx", "yz")
    (pair,) = small(pair_kernel, [(2, ROWS + EXTRA, width)], one, two)
    ring_one = [hop(v, "y", "x+") for v in (mine, pair, opposite)]
    ring_two = [hop(v, "z", "x-") for v in (mine, pair, opposite)]
    far_ones = [
        hop(ring_one[0], "z", "x+"), hop(ring_two[1], "y", "x-"), hop(ring_one[2], "z", "x+")
    ]
    tiles = {(0, 0): (mine, None), (0, 1): (one, None), (0, 2): (two, None), (0, 3): (opposite, None)}
    for m, ring in enumerate((ring_one, ring_two, far_ones), 1):
        tiles[m, 0], tiles[m, 3] = (ring[0], None), (ring[2], None)
        tiles[m, 1], tiles[m, 2] = (ring[1], 0), (ring[1], 1)

    sums_shape = (2 * router_weight.shape[1], tokens.shape[0])
    weights = (gate_other, up_other, gate_own, up_own)
    acc, squares, sums, down_own = early_of(gain, tiles, weights, down_proj, sums_shape)
    hidden, sums = late_of(gain, tiles, weights, acc, squares, sums)
    sums = along_z(sums, 0)

    places = [(0, 0), (0, ROWS), (1, 0), (1, ROWS)]
    far = down_of(True, [2 * ROWS] * 2, places, hidden, down_own, down_other)
    places = [(a, 0) for a in range(4)]
    places += [(4, 0), (5, 0), (8, 0), (8, ROWS)]
    places += [(9, 0), (10, 0), (6, 0), (7, 0)]
    shapes = [ROWS] * 8 + [2 * ROWS] + [ROWS] * 2
    rest = down_of(False, shapes, places, hidden, down_own, down_other)
    own, near, pair, singles = rest[:4], rest[4:8], rest[8], rest[9:]
    far_pairs = [hop(far[0], "z", "x-"), hop(far[1], "y", "x+")]
    far_in = [(far_pairs[n >> 1], (n & 1) * ROWS) for n in range(4)]
    pair_in = hop(pair, "y", "x-")
    singles_in = [hop(singles[n], "z", "x+") for n in range(2)]
    ways = [("y", "x-"), ("y", "x-"), ("z", "x+"), ("z", "x+")]
    near_in = [hop(added(near[n], far_in[n]), *ways[n]) for n in range(4)]
    parts = [
        (own[0], near_in[0], singles_in[0]),
        (own[1], near_in[1], singles_in[1]),
        (own[2], near_in[2], (pair_in, 0)),
        (own[3], near_in[3], (pair_in, ROWS)),
    ]
    terms = [
        *parts[0],
        hop(added(*parts[1]), "x-", "y"),
        hop(added(*parts[2]), "x+", "z"),
        hop(added(*parts[3]), "xx", "yz"),
    ]
    blocks = small(unpack_kernel, [block] * FAR, *terms)
    back = [along_z(blocks[k], (FAR - k) % FAR) for k in range(FAR)]
    keep, send = small(unshuffle_kernel, [kept, kept], *back)
    came = across_y(send)
    return pl.pallas_call(
        partial(combine_kernel, width_all),
        out_shape=jax.ShapeDtypeStruct(tokens.shape, BF16),
        in_specs=vmem(4),
        out_specs=vmem(1)[0],
        compiler_params=pltpu.CompilerParams(vmem_limit_bytes=4 << 20),
        name="combine",
    )(ids, sums, keep, came)


def solution(mesh):
    cut = Mesh(mesh.devices.reshape(SIZES), AXES)
    split = GRP + TP
    placed = (
        P(GRP, TP),
        P(),
        P(),
        P(GRP, None),
        P(None, split),
        P(None, split),
        P(split, None),
    )

    return jax.shard_map(per_device, mesh=cut, in_specs=placed, out_specs=P(GRP, TP), check_vma=False)
```

```python
from functools import partial

import jax
import jax.numpy as jnp
from jax import lax
from jax.experimental import pallas as pl
from jax.experimental.pallas import tpu as pltpu
from jax.sharding import Mesh
from jax.sharding import PartitionSpec as P


AXES = ("zh", "y2", "y1", "c", "zl", "x")
SIZES = (4, 2, 2, 2, 2, 4)
GRP = ("zh", "y2", "y1", "c")
TP = ("zl", "x")
OWNER = ("y1", "c", "zl", "x")
CAP = 18
FAR = 4
KEPT = FAR * CAP
ROWS = 2 * KEPT
NEAR = 56
CROSSED = 24
EXTRA = 8
BLOCK = 40
EPSILON = 1e-05
F32 = jnp.float32
BF16 = jnp.bfloat16


def place(y, z, x, step):
    if step == "x+":
        return y, z, (x + 1) % 4
    if step == "x-":
        return y, z, (x - 1) % 4
    if step == "xx":
        return y, z, (x + 2) % 4
    if step == "y":
        return 1 - y, z, x
    if step == "z":
        return y, 1 - z, x
    return 1 - y, 1 - z, x


def owner_pairs(*steps):
    pairs = []
    for y in range(2):
        for z in range(2):
            for x in range(4):
                for group, step in enumerate(steps):
                    ends = ((y, z, x), place(y, z, x, step))
                    pairs.append(
                        tuple(((j * 2 + (group ^ (j + k + n) & 1)) * 2 + k) * 4 + n for j, k, n in ends)
                    )
    return pairs


def hop(value, step_core0, step_core1):
    return lax.ppermute(value, OWNER, owner_pairs(step_core0, step_core1))


def along_z(value, distance):
    pairs = []
    for h in range(FAR):
        for c in range(2):
            for z in range(2):
                for x in range(4):
                    target = (h + distance) % FAR, c ^ (z + x) & 1
                    pairs.append(
                        tuple(((i * 2 + j) * 2 + z) * 4 + x for i, j in ((h, c), target))
                    )
    return lax.ppermute(value, ("zh", "c", "zl", "x"), pairs)


def across_y(value):
    pairs = [(i * 2 + c, (3 - i) * 2 + 1 - c) for i in range(4) for c in range(2)]
    return lax.ppermute(value, ("y2", "y1", "c"), pairs)


def other_core(value):
    return lax.ppermute(value, "c", [(0, 1), (1, 0)])


def vmem(count):
    return [pl.BlockSpec(memory_space=pltpu.VMEM)] * count


def hbm(count):
    return [pl.BlockSpec(memory_space=pltpu.HBM)] * count


def in_hbm(*arrays):
    return [pltpu.with_memory_space_constraint(a, pltpu.HBM) for a in arrays]


def small(kernel, outs, *operands):
    return pl.pallas_call(
        kernel,
        out_shape=[jax.ShapeDtypeStruct(shape, BF16) for shape in outs],
        in_specs=vmem(len(operands)),
        out_specs=vmem(len(outs)),
        compiler_params=pltpu.CompilerParams(vmem_limit_bytes=4 << 20),
    )(*operands)


def moved(shape, source_of, *blocks):
    joined = jnp.concatenate([b[...] for b in blocks], axis=0) if len(blocks) > 1 else blocks[0][...]
    row = lax.broadcasted_iota(jnp.int32, (shape[0], joined.shape[0]), 0)
    column = lax.broadcasted_iota(jnp.int32, (shape[0], joined.shape[0]), 1)
    source, valid = source_of(row)
    picks = jnp.where((source == column) & valid, 1.0, 0.0).astype(BF16)
    return jnp.dot(picks, joined, preferred_element_type=F32)


def leaving(row):
    part = jnp.where(row >= NEAR, 1, 0) + jnp.where(row >= 2 * NEAR, 1, 0)
    row = row - part * NEAR
    k = (row * 3641) >> 16
    half = jnp.where(part == 2, k, part)
    distance = jnp.where(part == 2, 2, jnp.where(k == 2, 3, k))
    return half, distance, row - k * CAP, k < jnp.where(part == 2, 2, 3)


def slots_of(ids):
    tokens = ids.shape[1]
    slot = lax.broadcasted_iota(jnp.int32, (2 * NEAR + BLOCK, tokens), 0)
    half, distance, inside, valid = leaving(slot)
    zh, y2 = lax.axis_index("zh"), lax.axis_index("y2")
    expert = ((zh + distance) & 3) * 2 + (y2 ^ half)
    first, second = ids[0:1, :] == expert, ids[1:2, :] == expert
    routed = jnp.where(first | second, 1.0, 0.0).astype(BF16)
    earlier = lax.broadcasted_iota(jnp.int32, (tokens, tokens), 0) < lax.broadcasted_iota(
        jnp.int32, (tokens, tokens), 1
    )
    before = jnp.dot(
        routed, jnp.where(earlier, 1.0, 0.0).astype(BF16), preferred_element_type=F32
    )
    here = (before == inside.astype(F32)) & valid
    return first & here, second & here


def select_kernel(ids_hbm, tokens_hbm, keep_ref, send_ref, far_ref, ids_ref, tokens_ref, sems):
    fetch = pltpu.make_async_copy(ids_hbm, ids_ref, sems.at[0])
    fetch_tokens = pltpu.make_async_copy(tokens_hbm, tokens_ref, sems.at[1])
    fetch.start()
    fetch_tokens.start()
    fetch.wait()
    first, second = slots_of(ids_ref[...])
    picks = jnp.where(first | second, 1.0, 0.0).astype(BF16)
    fetch_tokens.wait()
    chosen = jnp.dot(picks, tokens_ref[...], preferred_element_type=F32).astype(BF16)
    keep_ref[...] = chosen[:NEAR]
    send_ref[...] = chosen[NEAR : 2 * NEAR]
    far_ref[...] = chosen[2 * NEAR :]


def select(ids, tokens):
    sizes = (NEAR, NEAR, BLOCK)
    return pl.pallas_call(
        select_kernel,
        out_shape=[jax.ShapeDtypeStruct((n, tokens.shape[1]), BF16) for n in sizes],
        in_specs=hbm(2),
        out_specs=vmem(3),
        scratch_shapes=[
            pltpu.VMEM(ids.shape, ids.dtype),
            pltpu.VMEM(tokens.shape, BF16),
            pltpu.SemaphoreType.DMA((2,)),
        ],
        compiler_params=pltpu.CompilerParams(vmem_limit_bytes=4 << 20),
        name="select",
    )(*in_hbm(ids, tokens))


def in_blocks(row):
    block = (row * 1639) >> 16
    inside = row - block * BLOCK
    half = jnp.where(inside < CAP, 0, 1)
    return block, inside, half


def shuffle_kernel(keep_ref, came_ref, sums_ref, stay_ref, *out_refs):
    def source_of(row):
        block, inside, half = in_blocks(row)
        return half * NEAR + block * CAP + inside - half * CAP, inside < 2 * CAP

    rows = moved((3 * BLOCK, 0), source_of, keep_ref, came_ref)
    stay_ref[:BLOCK] = rows[:BLOCK].astype(BF16)
    stay_ref[BLOCK:] = sums_ref[...]
    for k, out in enumerate(out_refs, 1):
        out[...] = rows[k * BLOCK : (k + 1) * BLOCK].astype(BF16)


def cross_kernel(far_ref, out_ref):
    def source_of(row):
        return row + CAP, row < CAP

    out_ref[...] = moved((CROSSED, 0), source_of, far_ref).astype(BF16)


def pack_kernel(stay_ref, one_ref, two_ref, three_ref, crossed_ref, out_ref):
    start = BLOCK + EXTRA

    def source_of(row):
        block = (row * 1821) >> 16
        inside = row - block * 2 * CAP
        source = jnp.where(block == 0, 0, start + (block - 1) * BLOCK) + inside
        crossed = (block == 2) & (inside >= CAP)
        return jnp.where(crossed, start + 3 * BLOCK + inside - CAP, source), row >= 0

    refs = (stay_ref, one_ref, two_ref, three_ref, crossed_ref)
    out_ref[:ROWS] = moved((ROWS, 0), source_of, *refs).astype(BF16)
    out_ref[ROWS:] = stay_ref[BLOCK:]


def pair_kernel(first_ref, second_ref, out_ref):
    out_ref[0] = first_ref[...]
    out_ref[1] = second_ref[...]


def views(tiles, keys):
    arrays = []
    where = []
    for key in keys:
        array, at = tiles[key]
        known = [n for n, a in enumerate(arrays) if a is array]
        if not known:
            known = [len(arrays)]
            arrays.append(array)
        where.append((known[0], at))
    return arrays, where


def viewed(refs, where):
    return [refs[n] if at is None else refs[n].at[at] for n, at in where]


def unpack_kernel(*refs):
    terms, out_refs = refs[:-5], refs[-5:]
    total = sum(t[...].astype(F32) for t in terms).astype(BF16)

    def source_of(row):
        part, inside, _ = in_blocks(row)
        halves_row = row - 3 * BLOCK
        half = jnp.where(halves_row >= CROSSED, 1, 0)
        halves_row = halves_row - half * CROSSED
        block = jnp.where(part == 2, 3, part)
        near = row < 3 * BLOCK
        source = jnp.where(near, block * 2 * CAP + inside, (4 + half) * CAP + halves_row)
        return source, jnp.where(near, inside - 2 * CAP, halves_row - CAP) < 0

    rows = moved((3 * BLOCK + 2 * CROSSED, 0), source_of, total).astype(BF16)
    start = 0
    for out in out_refs:
        out[...] = rows[start : start + out.shape[0]]
        start += out.shape[0]


def join_kernel(keep_ref, came_ref, out_ref):
    def source_of(row):
        half = jnp.where(row < CAP, 0, 1)
        return half * CROSSED + row - half * CAP, row < 2 * CAP

    out_ref[...] = moved((BLOCK, 0), source_of, keep_ref, came_ref).astype(BF16)


def unshuffle_kernel(*refs):
    blocks, (keep_ref, send_ref) = refs[:3], refs[3:]

    def source_of(row):
        half = jnp.where(row < NEAR, 0, 1)
        row = row - half * NEAR
        k = (row * 3641) >> 16
        return k * BLOCK + half * CAP + row - k * CAP, k < 3

    rows = moved((2 * NEAR, 0), source_of, *blocks).astype(BF16)
    keep_ref[...] = rows[:NEAR]
    send_ref[...] = rows[NEAR:]


def transposed_dot(left, right):
    return lax.dot_general(left, right, (((1,), (1,)), ((), ())), preferred_element_type=F32)


def halves(value):
    high = value.astype(BF16)
    return high, (value - high.astype(F32)).astype(BF16)


def stats_kernel(tokens_hbm, gain_hbm, router_hbm, out_ref, gain_ref, tokens_ref, router_ref, sems):
    tokens, width = tokens_ref.shape
    part = lax.axis_index("zl") * 4 + lax.axis_index("x")
    here = pl.ds(pl.multiple_of(part * width, width), width)
    ways = ((tokens_hbm, tokens_ref), (gain_hbm, gain_ref), (router_hbm.at[:, here], router_ref))
    fetches = [pltpu.make_async_copy(a, b, sems.at[n]) for n, (a, b) in enumerate(ways)]
    for fetch in fetches:
        fetch.start()
    out_ref[...] = jnp.zeros_like(out_ref)
    for fetch in fetches:
        fetch.wait()
    values = tokens_ref[...].astype(F32)
    router = router_ref[...]
    ones = jnp.ones_like(router)
    scaled, squares = halves(values * gain_ref[:, here]), halves(values * values)
    for n, (left, terms) in enumerate(((router, scaled), (ones, squares))):
        for k, v in enumerate(halves(sum(transposed_dot(left, t) for t in terms))):
            start = (2 * n + k) * 128
            out_ref[:, start : start + tokens] = v


def stats(tokens, gain, router):
    width = tokens.shape[1]
    return pl.pallas_call(
        stats_kernel,
        out_shape=[
            jax.ShapeDtypeStruct((EXTRA, width), BF16),
            jax.ShapeDtypeStruct(gain.shape, F32),
        ],
        in_specs=hbm(3),
        out_specs=vmem(2),
        scratch_shapes=[
            pltpu.VMEM(tokens.shape, BF16),
            pltpu.VMEM((router.shape[0], width), BF16),
            pltpu.SemaphoreType.DMA((3,)),
        ],
        compiler_params=pltpu.CompilerParams(vmem_limit_bytes=4 << 20),
        name="stats",
    )(*in_hbm(tokens, gain, router))


def fetch_kernel(*refs):
    count = len(refs) // 2
    sems = refs[-1]
    copies = [
        pltpu.make_async_copy(refs[n], refs[count + n], sems.at[n]) for n in range(count)
    ]
    for copy in copies:
        copy.start()
    for copy in copies:
        copy.wait()


def fetched(*arrays):
    return pl.pallas_call(
        fetch_kernel,
        out_shape=[jax.ShapeDtypeStruct(a.shape, a.dtype) for a in arrays],
        in_specs=hbm(len(arrays)),
        out_specs=vmem(len(arrays)),
        scratch_shapes=[pltpu.SemaphoreType.DMA((len(arrays),))],
        compiler_params=pltpu.CompilerParams(vmem_limit_bytes=4 << 20),
        name="fetch",
    )(*in_hbm(*arrays))


def stats_in(tile, tokens):
    parts = [tile[ROWS:, n * 128 : n * 128 + tokens].astype(F32) for n in range(4)]
    return parts[0] + parts[1], parts[2] + parts[3]


def combine_kernel(width_all, ids_ref, sums_ref, keep_ref, came_ref, far_ref, out_ref):
    ids = ids_ref[...]
    sums = sums_ref[...]
    experts = sums.shape[0] // 2
    scale = lax.rsqrt(sums[experts : experts + 1] / width_all + EPSILON)
    named = lax.broadcasted_iota(jnp.int32, (experts, ids.shape[1]), 0)
    logits = [
        jnp.sum(jnp.where(named == ids[k : k + 1], sums[:experts], 0.0), axis=0, keepdims=True)
        * scale
        for k in (0, 1)
    ]
    gate_first = 1.0 / (1.0 + jnp.exp(logits[1] - logits[0]))
    gate_second = 1.0 / (1.0 + jnp.exp(logits[0] - logits[1]))
    first, second = slots_of(ids)
    weights = jnp.where(first, gate_first, 0.0) + jnp.where(second, gate_second, 0.0)
    rows = jnp.concatenate([keep_ref[...], came_ref[...], far_ref[...]], axis=0)
    out_ref[...] = sum(
        lax.dot_general(w, rows, (((0,), (0,)), ((), ())), preferred_element_type=F32)
        for w in halves(weights)
    ).astype(BF16)


def offset_place(square, ring):
    step = jnp.where(ring == 1, 3, jnp.where(ring == 2, 1, jnp.where(ring == 3, 2, 0)))
    feature = (lax.axis_index("zl") ^ (square >> 1)) * 4 + ((lax.axis_index("x") + step) & 3)
    return square & 1, feature


def group_index():
    place_sum = lax.axis_index("y1") + lax.axis_index("zl") + lax.axis_index("x")
    return lax.axis_index("c") ^ (place_sum & 1)


def tile_place(outer, inner):
    group = group_index()
    return offset_place(jnp.where(group == 0, outer, inner), jnp.where(group == 0, inner, outer))


CHUNK = 48
FIRST = ((0, 0), (0, 1), (0, 2), (0, 3), (1, 0), (1, 3), (2, 1), (2, 2))
SECOND = ((1, 1), (1, 2), (2, 0), (2, 3))
LAST = ((3, 0), (3, 1), (3, 2), (3, 3))


def prepare(tile, gain, out_ref, row_start, column_at, squares_ref, squares_start):
    width = tile.shape[1]

    def step(n, _):
        at = pl.multiple_of(n * CHUNK, CHUNK)
        values = tile[pl.ds(at, CHUNK), :].astype(F32)
        row_at = pl.ds(pl.multiple_of(row_start + at, 16), CHUNK)
        out_ref[row_at, column_at] = (values * gain).astype(BF16)
        square = values * values
        squares_at = pl.ds(pl.multiple_of(squares_start + at, 16), CHUNK)
        squares_ref[squares_at, :] += sum(
            square[:, j * 128 : (j + 1) * 128] for j in range(width // 128)
        )
        return 0

    lax.fori_loop(0, ROWS // CHUNK, step, 0)


def add_stats(tile, row_class, sums_ref):
    experts, tokens = sums_ref.shape[0] // 2, sums_ref.shape[1]
    own = jnp.where(row_class == 0, 1.0, 0.0)
    logits, squares = stats_in(tile, tokens)
    sums_ref[:experts] += logits * own
    sums_ref[experts:] += squares * own


def columns_of(feature, width):
    return pl.ds(pl.multiple_of(feature * width, width), width)


def place_tile(key, tile, gain_ref, x_ref, squares_ref, sums_ref):
    row_class, feature = tile_place(*key)
    column_at = columns_of(feature, tile.shape[1])
    start = row_class * ROWS
    prepare(tile, gain_ref[:, column_at], x_ref, start, column_at, squares_ref, start)
    add_stats(tile, row_class, sums_ref)


def fill_kernel(where, gain_ref, *refs):
    tiles, (x_ref, squares_ref, sums_ref) = viewed(refs, where), refs[-3:]
    width = tiles[0].shape[1]
    squares_ref[...] = jnp.zeros_like(squares_ref)
    sums_ref[...] = jnp.zeros_like(sums_ref)
    for key, tile in zip(FIRST, tiles):
        place_tile(key, tile, gain_ref, x_ref, squares_ref, sums_ref)
    for key in LAST:
        row_class, feature = tile_place(*key)
        row_at = pl.ds(pl.multiple_of(row_class * ROWS, ROWS), ROWS)
        x_ref[row_at, columns_of(feature, width)] = jnp.zeros((ROWS, width), BF16)


def early_kernel(where, gain_ref, *refs):
    tiles, weights, later = viewed(refs, where), refs[-14:-10], refs[-10]
    later_ref, acc_ref, x_ref, squares_ref, sums_ref, sem = refs[-6:]
    fetch = pltpu.make_async_copy(later, later_ref, sem.at[0])
    fetch.start()
    for key, tile in zip(SECOND, tiles):
        place_tile(key, tile, gain_ref, x_ref, squares_ref, sums_ref)
    for n, weight in enumerate(weights):
        acc_ref[n] = jnp.dot(x_ref[...], weight[...], preferred_element_type=F32)
    fetch.wait()


def early_of(gain, tiles, weights, later, sums_shape):
    width_all, slices = weights[0].shape
    given = [
        jax.ShapeDtypeStruct((2 * ROWS, width_all), BF16),
        jax.ShapeDtypeStruct((2 * ROWS, 128), F32),
        jax.ShapeDtypeStruct(sums_shape, F32),
    ]
    arrays, where = views(tiles, FIRST)
    filled = pl.pallas_call(
        partial(fill_kernel, where),
        out_shape=given,
        in_specs=vmem(1 + len(arrays)),
        out_specs=vmem(3),
        compiler_params=pltpu.CompilerParams(vmem_limit_bytes=8 << 20),
        name="fill",
    )(gain, *arrays)
    arrays, where = views(tiles, SECOND)
    at = 1 + len(arrays) + 5
    later_out, acc, _, squares, sums = pl.pallas_call(
        partial(early_kernel, where),
        out_shape=[
            jax.ShapeDtypeStruct(later.shape, later.dtype),
            jax.ShapeDtypeStruct((4, 2 * ROWS, slices), F32),
            *given,
        ],
        in_specs=vmem(at - 1) + hbm(1) + vmem(3),
        out_specs=vmem(5),
        input_output_aliases={at + n: 2 + n for n in range(3)},
        scratch_shapes=[pltpu.SemaphoreType.DMA((1,))],
        compiler_params=pltpu.CompilerParams(vmem_limit_bytes=12 << 20),
        cost_estimate=pl.CostEstimate(
            flops=2 * 2 * ROWS * width_all * 4 * slices,
            bytes_accessed=4 * width_all * slices * 2,
            transcendentals=0,
        ),
        name="early",
    )(gain, *arrays, *weights, *in_hbm(later), *filled)
    return acc, squares, sums, later_out


def late_kernel(width_all, where, gain_ref, *refs):
    tiles, weights = viewed(refs, where), refs[-12:-8]
    _, squares_in, sums_in, out_ref, sums_ref, acc_ref, squares_ref, x_ref = refs[-8:]
    width = tiles[0].shape[1]
    slices = weights[0].shape[1]
    squares_ref[...] = squares_in[...]
    sums_ref[...] = sums_in[...]
    for key, tile in zip(LAST, tiles):
        row_class, feature = tile_place(*key)
        column_at = columns_of(feature, width)
        start = row_class * ROWS
        gain = gain_ref[:, column_at]
        prepare(tile, gain, x_ref, 0, slice(None), squares_ref, start)
        add_stats(tile, row_class, sums_ref)
        row_at = pl.ds(pl.multiple_of(start, ROWS), ROWS)
        for n, weight in enumerate(weights):
            acc_ref[n, row_at, :] = acc_ref[n, row_at, :] + jnp.dot(
                x_ref[...], weight[column_at, :], preferred_element_type=F32
            )
    scale = lax.rsqrt(jnp.sum(squares_ref[...], axis=1, keepdims=True) / width_all + EPSILON)
    for half in range(2):
        gate, up = acc_ref[2 * half] * scale, acc_ref[2 * half + 1] * scale
        start = (1 - half) * slices
        out_ref[:, start : start + slices] = (gate * (1.0 / (1.0 + jnp.exp(-gate))) * up).astype(
            BF16
        )


def late_of(gain, tiles, weights, acc, squares, sums):
    width_all, slices = weights[0].shape
    arrays, where = views(tiles, LAST)
    width = arrays[0].shape[-1]
    at = 1 + len(arrays) + 4
    return pl.pallas_call(
        partial(late_kernel, width_all, where),
        out_shape=[
            jax.ShapeDtypeStruct((2 * ROWS, 2 * slices), BF16),
            jax.ShapeDtypeStruct(sums.shape, F32),
            jax.ShapeDtypeStruct(acc.shape, F32),
        ],
        in_specs=vmem(at + 3),
        out_specs=vmem(3),
        input_output_aliases={at: 2},
        scratch_shapes=[
            pltpu.VMEM(squares.shape, F32),
            pltpu.VMEM((ROWS, width), BF16),
        ],
        compiler_params=pltpu.CompilerParams(vmem_limit_bytes=12 << 20),
        cost_estimate=pl.CostEstimate(
            flops=2 * 4 * ROWS * width * 4 * slices,
            bytes_accessed=acc.size * 8,
            transcendentals=0,
        ),
        name="late",
    )(gain, *arrays, *weights, acc, squares, sums)[:2]


def down_kernel(far, places, hidden_ref, own_ref, other_ref, *refs):
    out_refs, y_ref = refs[:-1], refs[-1]
    slices = own_ref.shape[0]
    width = y_ref.shape[2]
    group = group_index()

    def product(rows, square, ring):
        _, feature = offset_place(square, ring)
        column_at = columns_of(feature, width)
        return (
            jnp.dot(hidden_ref[rows, :slices], own_ref[:, column_at], preferred_element_type=F32)
            + jnp.dot(hidden_ref[rows, slices:], other_ref[:, column_at], preferred_element_type=F32)
        ).astype(BF16)

    both, first, last = slice(None), slice(0, ROWS), slice(ROWS, 2 * ROWS)

    @pl.when(group == 0)
    def _():
        def step(ring, _):
            if far:
                y_ref[ring] = product(last, 3, ring)
                return 0
            pair = product(both, 0, ring)
            y_ref[ring] = pair[:ROWS]
            y_ref[4 + ring] = pair[ROWS:]
            y_ref[8 + ring] = product(first, 2, ring)
            return 0

        lax.fori_loop(0, 4, step, 0)

    @pl.when(group == 1)
    def _():
        def step(n, _):
            ring, square = (3, 2 * n) if far else (n >> 1, 2 * (n & 1))
            pair = product(both, square, ring)
            at = square if far else 4 * ring + square
            y_ref[at] = pair[:ROWS]
            y_ref[at + 1] = pair[ROWS:]
            return 0

        lax.fori_loop(0, 2 if far else 6, step, 0)

    for index, (at, start) in enumerate(places):
        out_refs[at][start : start + ROWS, :] = y_ref[index]


def down_of(far, shapes, places, hidden, own, other):
    slices, width_all = own.shape
    width = width_all // 8
    return pl.pallas_call(
        partial(down_kernel, far, places),
        out_shape=[jax.ShapeDtypeStruct((rows, width), BF16) for rows in shapes],
        in_specs=vmem(3),
        out_specs=vmem(len(shapes)),
        scratch_shapes=[pltpu.VMEM((len(places), ROWS, width), BF16)],
        compiler_params=pltpu.CompilerParams(vmem_limit_bytes=16 << 20),
        cost_estimate=pl.CostEstimate(
            flops=2 * len(places) * ROWS * width * 2 * slices,
            bytes_accessed=2 * slices * width_all * 2,
            transcendentals=0,
        ),
        name="far" if far else "rest",
    )(hidden, own, other)


def added_kernel(starts, *refs):
    *terms, out_ref = refs
    rows = out_ref.shape[0]
    out_ref[...] = sum(t[n : n + rows, :].astype(F32) for t, n in zip(terms, starts)).astype(BF16)


def added(*terms):
    terms = [t if isinstance(t, tuple) else (t, 0) for t in terms]
    (out,) = small(
        partial(added_kernel, [n for _, n in terms]),
        [(ROWS, terms[0][0].shape[1])],
        *(t for t, _ in terms),
    )
    return out


def per_device(tokens, norm_gain, router_weight, expert_ids, gate_proj, up_proj, down_proj):
    width_all = router_weight.shape[0]
    width = tokens.shape[1]
    gain = norm_gain.reshape(1, width_all)
    ids = expert_ids.T
    block = (BLOCK, width)

    keep, send, far = select(ids, tokens)
    part_sums, gain = stats(tokens, gain, router_weight.T)
    came = across_y(send)
    far = along_z(far, 2)
    stay, *blocks = small(
        shuffle_kernel, [(BLOCK + EXTRA, width), block, block], keep, came, part_sums
    )
    one, three = along_z(blocks[0], 1), along_z(blocks[1], 3)
    stay = along_z(stay, 0)
    (crossed,) = small(cross_kernel, [(CROSSED, width)], far)
    crossed = across_y(crossed)
    gate_other = other_core(gate_proj)
    up_other = other_core(up_proj)
    down_other = other_core(down_proj)
    (mine,) = small(pack_kernel, [(ROWS + EXTRA, width)], stay, one, far, three, crossed)
    gate_own, up_own = fetched(gate_proj, up_proj)

    one = hop(mine, "x+", "y")
    two = hop(mine, "x-", "z")
    opposite = hop(mine, "xx", "yz")
    (pair,) = small(pair_kernel, [(2, ROWS + EXTRA, width)], one, two)
    ring_one = [hop(v, "y", "x+") for v in (mine, pair, opposite)]
    ring_two = [hop(v, "z", "x-") for v in (mine, pair, opposite)]
    far_ones = [
        hop(ring_one[0], "z", "x+"), hop(ring_two[1], "y", "x-"), hop(ring_one[2], "z", "x+")
    ]
    tiles = {(0, 0): (mine, None), (0, 1): (one, None), (0, 2): (two, None), (0, 3): (opposite, None)}
    for m, ring in enumerate((ring_one, ring_two, far_ones), 1):
        tiles[m, 0], tiles[m, 3] = (ring[0], None), (ring[2], None)
        tiles[m, 1], tiles[m, 2] = (ring[1], 0), (ring[1], 1)

    sums_shape = (2 * router_weight.shape[1], tokens.shape[0])
    weights = (gate_other, up_other, gate_own, up_own)
    acc, squares, sums, down_own = early_of(gain, tiles, weights, down_proj, sums_shape)
    hidden, sums = late_of(gain, tiles, weights, acc, squares, sums)
    sums = along_z(sums, 0)

    places = [(0, 0), (0, ROWS), (1, 0), (1, ROWS)]
    far = down_of(True, [2 * ROWS] * 2, places, hidden, down_own, down_other)
    places = [(a, 0) for a in range(4)]
    places += [(4, 0), (5, 0), (8, 0), (8, ROWS)]
    places += [(9, 0), (10, 0), (6, 0), (7, 0)]
    shapes = [ROWS] * 8 + [2 * ROWS] + [ROWS] * 2
    rest = down_of(False, shapes, places, hidden, down_own, down_other)
    own, near, pair, singles = rest[:4], rest[4:8], rest[8], rest[9:]
    far_pairs = [hop(far[0], "z", "x-"), hop(far[1], "y", "x+")]
    far_in = [(far_pairs[n >> 1], (n & 1) * ROWS) for n in range(4)]
    pair_in = hop(pair, "y", "x-")
    singles_in = [hop(singles[n], "z", "x+") for n in range(2)]
    ways = [("y", "x-"), ("y", "x-"), ("z", "x+"), ("z", "x+")]
    near_in = [hop(added(near[n], far_in[n]), *ways[n]) for n in range(4)]
    parts = [
        (own[0], near_in[0], singles_in[0]),
        (own[1], near_in[1], singles_in[1]),
        (own[2], near_in[2], (pair_in, 0)),
        (own[3], near_in[3], (pair_in, ROWS)),
    ]
    terms = [
        *parts[0],
        hop(added(*parts[1]), "x-", "y"),
        hop(added(*parts[2]), "x+", "z"),
        hop(added(*parts[3]), "xx", "yz"),
    ]
    crossed = (CROSSED, width)
    stay, one, three, two, other = small(unpack_kernel, [block] * 3 + [crossed] * 2, *terms)
    other = across_y(other)
    one, three = along_z(one, 3), along_z(three, 1)
    stay = along_z(stay, 0)
    (far,) = small(join_kernel, [block], two, other)
    far = along_z(far, 2)
    keep, send = small(unshuffle_kernel, [(NEAR, width)] * 2, stay, one, three)
    came = across_y(send)
    return pl.pallas_call(
        partial(combine_kernel, width_all),
        out_shape=jax.ShapeDtypeStruct(tokens.shape, BF16),
        in_specs=vmem(5),
        out_specs=vmem(1)[0],
        compiler_params=pltpu.CompilerParams(vmem_limit_bytes=4 << 20),
        name="combine",
    )(ids, sums, keep, came, far)


def solution(mesh):
    cut = Mesh(mesh.devices.reshape(SIZES), AXES)
    split = GRP + TP
    placed = (
        P(GRP, TP),
        P(),
        P(),
        P(GRP, None),
        P(None, split),
        P(None, split),
        P(split, None),
    )

    return jax.shard_map(per_device, mesh=cut, in_specs=placed, out_specs=P(GRP, TP), check_vma=False)
```

```python
from functools import partial

import jax
import jax.numpy as jnp
from jax import lax
from jax.experimental import pallas as pl
from jax.experimental.pallas import tpu as pltpu
from jax.sharding import Mesh
from jax.sharding import PartitionSpec as P


AXES = ("zh", "y2", "y1", "c", "zl", "x")
SIZES = (4, 2, 2, 2, 2, 4)
GRP = ("zh", "y2", "y1", "c")
TP = ("zl", "x")
OWNER = ("y1", "c", "zl", "x")
CAP = 18
FAR = 4
KEPT = FAR * CAP
ROWS = 2 * KEPT
NEAR = 56
CROSSED = 24
EXTRA = 8
BLOCK = 40
EPSILON = 1e-05
F32 = jnp.float32
BF16 = jnp.bfloat16


def place(y, z, x, step):
    if step == "x+":
        return y, z, (x + 1) % 4
    if step == "x-":
        return y, z, (x - 1) % 4
    if step == "xx":
        return y, z, (x + 2) % 4
    if step == "y":
        return 1 - y, z, x
    if step == "z":
        return y, 1 - z, x
    return 1 - y, 1 - z, x


def owner_pairs(*steps):
    pairs = []
    for y in range(2):
        for z in range(2):
            for x in range(4):
                for group, step in enumerate(steps):
                    ends = ((y, z, x), place(y, z, x, step))
                    pairs.append(
                        tuple(((j * 2 + (group ^ (j + k + n) & 1)) * 2 + k) * 4 + n for j, k, n in ends)
                    )
    return pairs


def hop(value, step_core0, step_core1):
    return lax.ppermute(value, OWNER, owner_pairs(step_core0, step_core1))


def along_z(value, distance):
    pairs = []
    for h in range(FAR):
        for c in range(2):
            for z in range(2):
                for x in range(4):
                    target = (h + distance) % FAR, c ^ (z + x) & 1
                    pairs.append(
                        tuple(((i * 2 + j) * 2 + z) * 4 + x for i, j in ((h, c), target))
                    )
    return lax.ppermute(value, ("zh", "c", "zl", "x"), pairs)


def across_y(value):
    pairs = [(i * 2 + c, (3 - i) * 2 + 1 - c) for i in range(4) for c in range(2)]
    return lax.ppermute(value, ("y2", "y1", "c"), pairs)


def other_core(value):
    return lax.ppermute(value, "c", [(0, 1), (1, 0)])


def vmem(count):
    return [pl.BlockSpec(memory_space=pltpu.VMEM)] * count


def hbm(count):
    return [pl.BlockSpec(memory_space=pltpu.HBM)] * count


def in_hbm(*arrays):
    return [pltpu.with_memory_space_constraint(a, pltpu.HBM) for a in arrays]


def small(kernel, outs, *operands):
    return pl.pallas_call(
        kernel,
        out_shape=[jax.ShapeDtypeStruct(shape, BF16) for shape in outs],
        in_specs=vmem(len(operands)),
        out_specs=vmem(len(outs)),
        compiler_params=pltpu.CompilerParams(vmem_limit_bytes=4 << 20),
    )(*operands)


def moved(shape, source_of, *blocks):
    joined = jnp.concatenate([b[...] for b in blocks], axis=0) if len(blocks) > 1 else blocks[0][...]
    row = lax.broadcasted_iota(jnp.int32, (shape[0], joined.shape[0]), 0)
    column = lax.broadcasted_iota(jnp.int32, (shape[0], joined.shape[0]), 1)
    source, valid = source_of(row)
    picks = jnp.where((source == column) & valid, 1.0, 0.0).astype(BF16)
    return jnp.dot(picks, joined, preferred_element_type=F32)


def leaving(row):
    part = jnp.where(row >= NEAR, 1, 0) + jnp.where(row >= 2 * NEAR, 1, 0)
    row = row - part * NEAR
    k = (row * 3641) >> 16
    half = jnp.where(part == 2, k, part)
    distance = jnp.where(part == 2, 2, jnp.where(k == 2, 3, k))
    return half, distance, row - k * CAP, k < jnp.where(part == 2, 2, 3)


def slots_of(ids):
    tokens = ids.shape[1]
    slot = lax.broadcasted_iota(jnp.int32, (2 * NEAR + BLOCK, tokens), 0)
    half, distance, inside, valid = leaving(slot)
    zh, y2 = lax.axis_index("zh"), lax.axis_index("y2")
    expert = ((zh + distance) & 3) * 2 + (y2 ^ half)
    first, second = ids[0:1, :] == expert, ids[1:2, :] == expert
    routed = jnp.where(first | second, 1.0, 0.0).astype(BF16)
    earlier = lax.broadcasted_iota(jnp.int32, (tokens, tokens), 0) < lax.broadcasted_iota(
        jnp.int32, (tokens, tokens), 1
    )
    before = jnp.dot(
        routed, jnp.where(earlier, 1.0, 0.0).astype(BF16), preferred_element_type=F32
    )
    here = (before == inside.astype(F32)) & valid
    return first & here, second & here


def select_kernel(ids_hbm, tokens_hbm, keep_ref, send_ref, far_ref, ids_ref, tokens_ref, sems):
    fetch = pltpu.make_async_copy(ids_hbm, ids_ref, sems.at[0])
    fetch_tokens = pltpu.make_async_copy(tokens_hbm, tokens_ref, sems.at[1])
    fetch.start()
    fetch_tokens.start()
    fetch.wait()
    first, second = slots_of(ids_ref[...])
    picks = jnp.where(first | second, 1.0, 0.0).astype(BF16)
    fetch_tokens.wait()
    chosen = jnp.dot(picks, tokens_ref[...], preferred_element_type=F32).astype(BF16)
    keep_ref[...] = chosen[:NEAR]
    send_ref[...] = chosen[NEAR : 2 * NEAR]
    far_ref[...] = chosen[2 * NEAR :]


def select(ids, tokens):
    sizes = (NEAR, NEAR, BLOCK)
    return pl.pallas_call(
        select_kernel,
        out_shape=[jax.ShapeDtypeStruct((n, tokens.shape[1]), BF16) for n in sizes],
        in_specs=hbm(2),
        out_specs=vmem(3),
        scratch_shapes=[
            pltpu.VMEM(ids.shape, ids.dtype),
            pltpu.VMEM(tokens.shape, BF16),
            pltpu.SemaphoreType.DMA((2,)),
        ],
        compiler_params=pltpu.CompilerParams(vmem_limit_bytes=4 << 20),
        name="select",
    )(*in_hbm(ids, tokens))


def in_blocks(row):
    block = (row * 1639) >> 16
    inside = row - block * BLOCK
    half = jnp.where(inside < CAP, 0, 1)
    return block, inside, half


def shuffle_kernel(keep_ref, came_ref, sums_ref, stay_ref, *out_refs):
    def source_of(row):
        block, inside, half = in_blocks(row)
        return half * NEAR + block * CAP + inside - half * CAP, inside < 2 * CAP

    rows = moved((3 * BLOCK, 0), source_of, keep_ref, came_ref)
    stay_ref[:BLOCK] = rows[:BLOCK].astype(BF16)
    stay_ref[BLOCK:] = sums_ref[...]
    for k, out in enumerate(out_refs, 1):
        out[...] = rows[k * BLOCK : (k + 1) * BLOCK].astype(BF16)


def cross_kernel(far_ref, out_ref):
    def source_of(row):
        return row + CAP, row < CAP

    out_ref[...] = moved((CROSSED, 0), source_of, far_ref).astype(BF16)


def pack_kernel(stay_ref, one_ref, two_ref, three_ref, crossed_ref, out_ref):
    start = BLOCK + EXTRA

    def source_of(row):
        block = (row * 1821) >> 16
        inside = row - block * 2 * CAP
        source = jnp.where(block == 0, 0, start + (block - 1) * BLOCK) + inside
        crossed = (block == 2) & (inside >= CAP)
        return jnp.where(crossed, start + 3 * BLOCK + inside - CAP, source), row >= 0

    refs = (stay_ref, one_ref, two_ref, three_ref, crossed_ref)
    out_ref[:ROWS] = moved((ROWS, 0), source_of, *refs).astype(BF16)
    out_ref[ROWS:] = stay_ref[BLOCK:]


def pair_kernel(first_ref, second_ref, out_ref):
    out_ref[0] = first_ref[...]
    out_ref[1] = second_ref[...]


def views(tiles, keys):
    arrays = []
    where = []
    for key in keys:
        array, at = tiles[key]
        known = [n for n, a in enumerate(arrays) if a is array]
        if not known:
            known = [len(arrays)]
            arrays.append(array)
        where.append((known[0], at))
    return arrays, where


def viewed(refs, where):
    return [refs[n] if at is None else refs[n].at[at] for n, at in where]


def unpack_kernel(*refs):
    terms, out_refs = refs[:-5], refs[-5:]
    total = sum(t[...].astype(F32) for t in terms).astype(BF16)

    def source_of(row):
        part, inside, _ = in_blocks(row)
        halves_row = row - 3 * BLOCK
        half = jnp.where(halves_row >= CROSSED, 1, 0)
        halves_row = halves_row - half * CROSSED
        block = jnp.where(part == 2, 3, part)
        near = row < 3 * BLOCK
        source = jnp.where(near, block * 2 * CAP + inside, (4 + half) * CAP + halves_row)
        return source, jnp.where(near, inside - 2 * CAP, halves_row - CAP) < 0

    rows = moved((3 * BLOCK + 2 * CROSSED, 0), source_of, total).astype(BF16)
    start = 0
    for out in out_refs:
        out[...] = rows[start : start + out.shape[0]]
        start += out.shape[0]


def join_kernel(keep_ref, came_ref, out_ref):
    def source_of(row):
        half = jnp.where(row < CAP, 0, 1)
        return half * CROSSED + row - half * CAP, row < 2 * CAP

    out_ref[...] = moved((BLOCK, 0), source_of, keep_ref, came_ref).astype(BF16)


def unshuffle_kernel(*refs):
    blocks, (keep_ref, send_ref) = refs[:3], refs[3:]

    def source_of(row):
        half = jnp.where(row < NEAR, 0, 1)
        row = row - half * NEAR
        k = (row * 3641) >> 16
        return k * BLOCK + half * CAP + row - k * CAP, k < 3

    rows = moved((2 * NEAR, 0), source_of, *blocks).astype(BF16)
    keep_ref[...] = rows[:NEAR]
    send_ref[...] = rows[NEAR:]


def transposed_dot(left, right):
    return lax.dot_general(left, right, (((1,), (1,)), ((), ())), preferred_element_type=F32)


def halves(value):
    high = value.astype(BF16)
    return high, (value - high.astype(F32)).astype(BF16)


def stats_kernel(tokens_hbm, gain_hbm, router_hbm, out_ref, gain_ref, tokens_ref, router_ref, sems):
    tokens, width = tokens_ref.shape
    part = lax.axis_index("zl") * 4 + lax.axis_index("x")
    here = pl.ds(pl.multiple_of(part * width, width), width)
    ways = ((tokens_hbm, tokens_ref), (gain_hbm, gain_ref), (router_hbm.at[:, here], router_ref))
    fetches = [pltpu.make_async_copy(a, b, sems.at[n]) for n, (a, b) in enumerate(ways)]
    for fetch in fetches:
        fetch.start()
    out_ref[...] = jnp.zeros_like(out_ref)
    for fetch in fetches:
        fetch.wait()
    values = tokens_ref[...].astype(F32)
    router = router_ref[...]
    ones = jnp.ones_like(router)
    scaled, squares = halves(values * gain_ref[:, here]), halves(values * values)
    for n, (left, terms) in enumerate(((router, scaled), (ones, squares))):
        for k, v in enumerate(halves(sum(transposed_dot(left, t) for t in terms))):
            start = (2 * n + k) * 128
            out_ref[:, start : start + tokens] = v


def stats(tokens, gain, router):
    width = tokens.shape[1]
    return pl.pallas_call(
        stats_kernel,
        out_shape=[
            jax.ShapeDtypeStruct((EXTRA, width), BF16),
            jax.ShapeDtypeStruct(gain.shape, F32),
        ],
        in_specs=hbm(3),
        out_specs=vmem(2),
        scratch_shapes=[
            pltpu.VMEM(tokens.shape, BF16),
            pltpu.VMEM((router.shape[0], width), BF16),
            pltpu.SemaphoreType.DMA((3,)),
        ],
        compiler_params=pltpu.CompilerParams(vmem_limit_bytes=4 << 20),
        name="stats",
    )(*in_hbm(tokens, gain, router))


def fetch_kernel(*refs):
    count = len(refs) // 2
    sems = refs[-1]
    copies = [
        pltpu.make_async_copy(refs[n], refs[count + n], sems.at[n]) for n in range(count)
    ]
    for copy in copies:
        copy.start()
    for copy in copies:
        copy.wait()


def fetched(*arrays):
    return pl.pallas_call(
        fetch_kernel,
        out_shape=[jax.ShapeDtypeStruct(a.shape, a.dtype) for a in arrays],
        in_specs=hbm(len(arrays)),
        out_specs=vmem(len(arrays)),
        scratch_shapes=[pltpu.SemaphoreType.DMA((len(arrays),))],
        compiler_params=pltpu.CompilerParams(vmem_limit_bytes=4 << 20),
        name="fetch",
    )(*in_hbm(*arrays))


def stats_in(tile, tokens):
    parts = [tile[ROWS:, n * 128 : n * 128 + tokens].astype(F32) for n in range(4)]
    return parts[0] + parts[1], parts[2] + parts[3]


def gates_kernel(width_all, ids_ref, sums_ref, *out_refs):
    ids = ids_ref[...]
    sums = sums_ref[...]
    experts = sums.shape[0] // 2
    scale = lax.rsqrt(sums[experts : experts + 1] / width_all + EPSILON)
    named = lax.broadcasted_iota(jnp.int32, (experts, ids.shape[1]), 0)
    logits = [
        jnp.sum(jnp.where(named == ids[k : k + 1], sums[:experts], 0.0), axis=0, keepdims=True)
        * scale
        for k in (0, 1)
    ]
    gate_first = 1.0 / (1.0 + jnp.exp(logits[1] - logits[0]))
    gate_second = 1.0 / (1.0 + jnp.exp(logits[0] - logits[1]))
    first, second = slots_of(ids)
    weights = jnp.where(first, gate_first, 0.0) + jnp.where(second, gate_second, 0.0)
    for out, part in zip(out_refs, halves(weights)):
        out[...] = part


def combine_kernel(high_ref, low_ref, keep_ref, came_ref, far_ref, out_ref):
    rows = jnp.concatenate([keep_ref[...], came_ref[...], far_ref[...]], axis=0)
    out_ref[...] = sum(
        lax.dot_general(w[...], rows, (((0,), (0,)), ((), ())), preferred_element_type=F32)
        for w in (high_ref, low_ref)
    ).astype(BF16)


def offset_place(square, ring):
    step = jnp.where(ring == 1, 3, jnp.where(ring == 2, 1, jnp.where(ring == 3, 2, 0)))
    feature = (lax.axis_index("zl") ^ (square >> 1)) * 4 + ((lax.axis_index("x") + step) & 3)
    return square & 1, feature


def group_index():
    place_sum = lax.axis_index("y1") + lax.axis_index("zl") + lax.axis_index("x")
    return lax.axis_index("c") ^ (place_sum & 1)


def tile_place(outer, inner):
    group = group_index()
    return offset_place(jnp.where(group == 0, outer, inner), jnp.where(group == 0, inner, outer))


CHUNK = 48
FIRST = ((0, 0), (0, 1), (0, 2), (0, 3), (1, 0), (1, 3), (2, 1), (2, 2))
SECOND = ((1, 1), (1, 2), (2, 0), (2, 3), (3, 0))
LAST = ((3, 1), (3, 2), (3, 3))


def prepare(tile, gain, out_ref, row_start, column_at, squares_ref, squares_start):
    width = tile.shape[1]

    def step(n, _):
        at = pl.multiple_of(n * CHUNK, CHUNK)
        values = tile[pl.ds(at, CHUNK), :].astype(F32)
        row_at = pl.ds(pl.multiple_of(row_start + at, 16), CHUNK)
        out_ref[row_at, column_at] = (values * gain).astype(BF16)
        square = values * values
        squares_at = pl.ds(pl.multiple_of(squares_start + at, 16), CHUNK)
        squares_ref[squares_at, :] += sum(
            square[:, j * 128 : (j + 1) * 128] for j in range(width // 128)
        )
        return 0

    lax.fori_loop(0, ROWS // CHUNK, step, 0)


def add_stats(tile, row_class, sums_ref):
    experts, tokens = sums_ref.shape[0] // 2, sums_ref.shape[1]
    own = jnp.where(row_class == 0, 1.0, 0.0)
    logits, squares = stats_in(tile, tokens)
    sums_ref[:experts] += logits * own
    sums_ref[experts:] += squares * own


def columns_of(feature, width):
    return pl.ds(pl.multiple_of(feature * width, width), width)


def place_tile(key, tile, gain_ref, x_ref, squares_ref, sums_ref):
    row_class, feature = tile_place(*key)
    column_at = columns_of(feature, tile.shape[1])
    start = row_class * ROWS
    prepare(tile, gain_ref[:, column_at], x_ref, start, column_at, squares_ref, start)
    add_stats(tile, row_class, sums_ref)


def fill_kernel(where, gain_ref, *refs):
    tiles, (x_ref, squares_ref, sums_ref) = viewed(refs, where), refs[-3:]
    width = tiles[0].shape[1]
    squares_ref[...] = jnp.zeros_like(squares_ref)
    sums_ref[...] = jnp.zeros_like(sums_ref)
    for key, tile in zip(FIRST, tiles):
        place_tile(key, tile, gain_ref, x_ref, squares_ref, sums_ref)
    for key in LAST:
        row_class, feature = tile_place(*key)
        row_at = pl.ds(pl.multiple_of(row_class * ROWS, ROWS), ROWS)
        x_ref[row_at, columns_of(feature, width)] = jnp.zeros((ROWS, width), BF16)


def early_kernel(where, gain_ref, *refs):
    tiles, weights, later = viewed(refs, where), refs[-14:-10], refs[-10]
    later_ref, acc_ref, x_ref, squares_ref, sums_ref, sem = refs[-6:]
    fetch = pltpu.make_async_copy(later, later_ref, sem.at[0])
    fetch.start()
    for key, tile in zip(SECOND, tiles):
        place_tile(key, tile, gain_ref, x_ref, squares_ref, sums_ref)
    for n, weight in enumerate(weights):
        acc_ref[n] = jnp.dot(x_ref[...], weight[...], preferred_element_type=F32)
    fetch.wait()


def early_of(gain, tiles, weights, later, sums_shape):
    width_all, slices = weights[0].shape
    given = [
        jax.ShapeDtypeStruct((2 * ROWS, width_all), BF16),
        jax.ShapeDtypeStruct((2 * ROWS, 128), F32),
        jax.ShapeDtypeStruct(sums_shape, F32),
    ]
    arrays, where = views(tiles, FIRST)
    filled = pl.pallas_call(
        partial(fill_kernel, where),
        out_shape=given,
        in_specs=vmem(1 + len(arrays)),
        out_specs=vmem(3),
        compiler_params=pltpu.CompilerParams(vmem_limit_bytes=8 << 20),
        name="fill",
    )(gain, *arrays)
    arrays, where = views(tiles, SECOND)
    at = 1 + len(arrays) + 5
    later_out, acc, _, squares, sums = pl.pallas_call(
        partial(early_kernel, where),
        out_shape=[
            jax.ShapeDtypeStruct(later.shape, later.dtype),
            jax.ShapeDtypeStruct((4, 2 * ROWS, slices), F32),
            *given,
        ],
        in_specs=vmem(at - 1) + hbm(1) + vmem(3),
        out_specs=vmem(5),
        input_output_aliases={at + n: 2 + n for n in range(3)},
        scratch_shapes=[pltpu.SemaphoreType.DMA((1,))],
        compiler_params=pltpu.CompilerParams(vmem_limit_bytes=12 << 20),
        cost_estimate=pl.CostEstimate(
            flops=2 * 2 * ROWS * width_all * 4 * slices,
            bytes_accessed=4 * width_all * slices * 2,
            transcendentals=0,
        ),
        name="early",
    )(gain, *arrays, *weights, *in_hbm(later), *filled)
    return acc, squares, sums, later_out


def late_kernel(width_all, where, gain_ref, *refs):
    tiles, weights = viewed(refs, where), refs[-12:-8]
    _, squares_in, sums_in, out_ref, sums_ref, acc_ref, squares_ref, x_ref = refs[-8:]
    width = tiles[0].shape[1]
    slices = weights[0].shape[1]
    squares_ref[...] = squares_in[...]
    sums_ref[...] = sums_in[...]
    for key, tile in zip(LAST, tiles):
        row_class, feature = tile_place(*key)
        column_at = columns_of(feature, width)
        start = row_class * ROWS
        gain = gain_ref[:, column_at]
        prepare(tile, gain, x_ref, 0, slice(None), squares_ref, start)
        add_stats(tile, row_class, sums_ref)
        row_at = pl.ds(pl.multiple_of(start, ROWS), ROWS)
        for n, weight in enumerate(weights):
            acc_ref[n, row_at, :] = acc_ref[n, row_at, :] + jnp.dot(
                x_ref[...], weight[column_at, :], preferred_element_type=F32
            )
    scale = lax.rsqrt(jnp.sum(squares_ref[...], axis=1, keepdims=True) / width_all + EPSILON)
    for half in range(2):
        gate, up = acc_ref[2 * half] * scale, acc_ref[2 * half + 1] * scale
        start = (1 - half) * slices
        out_ref[:, start : start + slices] = (gate * (1.0 / (1.0 + jnp.exp(-gate))) * up).astype(
            BF16
        )


def late_of(gain, tiles, weights, acc, squares, sums):
    width_all, slices = weights[0].shape
    arrays, where = views(tiles, LAST)
    width = arrays[0].shape[-1]
    at = 1 + len(arrays) + 4
    return pl.pallas_call(
        partial(late_kernel, width_all, where),
        out_shape=[
            jax.ShapeDtypeStruct((2 * ROWS, 2 * slices), BF16),
            jax.ShapeDtypeStruct(sums.shape, F32),
            jax.ShapeDtypeStruct(acc.shape, F32),
        ],
        in_specs=vmem(at + 3),
        out_specs=vmem(3),
        input_output_aliases={at: 2},
        scratch_shapes=[
            pltpu.VMEM(squares.shape, F32),
            pltpu.VMEM((ROWS, width), BF16),
        ],
        compiler_params=pltpu.CompilerParams(vmem_limit_bytes=12 << 20),
        cost_estimate=pl.CostEstimate(
            flops=2 * 4 * ROWS * width * 4 * slices,
            bytes_accessed=acc.size * 8,
            transcendentals=0,
        ),
        name="late",
    )(gain, *arrays, *weights, acc, squares, sums)[:2]


def down_kernel(far, places, hidden_ref, own_ref, other_ref, *refs):
    out_refs, y_ref = refs[:-1], refs[-1]
    slices = own_ref.shape[0]
    width = y_ref.shape[2]
    group = group_index()

    def product(rows, square, ring):
        _, feature = offset_place(square, ring)
        column_at = columns_of(feature, width)
        return (
            jnp.dot(hidden_ref[rows, :slices], own_ref[:, column_at], preferred_element_type=F32)
            + jnp.dot(hidden_ref[rows, slices:], other_ref[:, column_at], preferred_element_type=F32)
        ).astype(BF16)

    both, first, last = slice(None), slice(0, ROWS), slice(ROWS, 2 * ROWS)

    @pl.when(group == 0)
    def _():
        def step(ring, _):
            if far:
                y_ref[ring] = product(last, 3, ring)
                return 0
            pair = product(both, 0, ring)
            y_ref[ring] = pair[:ROWS]
            y_ref[4 + ring] = pair[ROWS:]
            y_ref[8 + ring] = product(first, 2, ring)
            return 0

        lax.fori_loop(0, 4, step, 0)

    @pl.when(group == 1)
    def _():
        def step(n, _):
            ring, square = (3, 2 * n) if far else (n >> 1, 2 * (n & 1))
            pair = product(both, square, ring)
            at = square if far else 4 * ring + square
            y_ref[at] = pair[:ROWS]
            y_ref[at + 1] = pair[ROWS:]
            return 0

        lax.fori_loop(0, 2 if far else 6, step, 0)

    for index, (at, start) in enumerate(places):
        out_refs[at][start : start + ROWS, :] = y_ref[index]


def down_of(far, shapes, places, hidden, own, other):
    slices, width_all = own.shape
    width = width_all // 8
    return pl.pallas_call(
        partial(down_kernel, far, places),
        out_shape=[jax.ShapeDtypeStruct((rows, width), BF16) for rows in shapes],
        in_specs=vmem(3),
        out_specs=vmem(len(shapes)),
        scratch_shapes=[pltpu.VMEM((len(places), ROWS, width), BF16)],
        compiler_params=pltpu.CompilerParams(vmem_limit_bytes=16 << 20),
        cost_estimate=pl.CostEstimate(
            flops=2 * len(places) * ROWS * width * 2 * slices,
            bytes_accessed=2 * slices * width_all * 2,
            transcendentals=0,
        ),
        name="far" if far else "rest",
    )(hidden, own, other)


def added_kernel(starts, *refs):
    *terms, out_ref = refs
    rows = out_ref.shape[0]
    out_ref[...] = sum(t[n : n + rows, :].astype(F32) for t, n in zip(terms, starts)).astype(BF16)


def added(*terms):
    terms = [t if isinstance(t, tuple) else (t, 0) for t in terms]
    (out,) = small(
        partial(added_kernel, [n for _, n in terms]),
        [(ROWS, terms[0][0].shape[1])],
        *(t for t, _ in terms),
    )
    return out


def per_device(tokens, norm_gain, router_weight, expert_ids, gate_proj, up_proj, down_proj):
    width_all = router_weight.shape[0]
    width = tokens.shape[1]
    gain = norm_gain.reshape(1, width_all)
    ids = expert_ids.T
    block = (BLOCK, width)

    keep, send, far = select(ids, tokens)
    part_sums, gain = stats(tokens, gain, router_weight.T)
    came = across_y(send)
    far = along_z(far, 2)
    stay, *blocks = small(
        shuffle_kernel, [(BLOCK + EXTRA, width), block, block], keep, came, part_sums
    )
    one, three = along_z(blocks[0], 1), along_z(blocks[1], 3)
    stay = along_z(stay, 0)
    (crossed,) = small(cross_kernel, [(CROSSED, width)], far)
    crossed = across_y(crossed)
    gate_other = other_core(gate_proj)
    up_other = other_core(up_proj)
    down_other = other_core(down_proj)
    (mine,) = small(pack_kernel, [(ROWS + EXTRA, width)], stay, one, far, three, crossed)
    gate_own, up_own = fetched(gate_proj, up_proj)

    one = hop(mine, "x+", "y")
    two = hop(mine, "x-", "z")
    opposite = hop(mine, "xx", "yz")
    (pair,) = small(pair_kernel, [(2, ROWS + EXTRA, width)], one, two)
    ring_one = [hop(v, "y", "x+") for v in (mine, pair, opposite)]
    ring_two = [hop(v, "z", "x-") for v in (mine, pair, opposite)]
    far_ones = [
        hop(ring_one[0], "z", "x+"), hop(ring_two[1], "y", "x-"), hop(ring_one[2], "z", "x+")
    ]
    tiles = {(0, 0): (mine, None), (0, 1): (one, None), (0, 2): (two, None), (0, 3): (opposite, None)}
    for m, ring in enumerate((ring_one, ring_two, far_ones), 1):
        tiles[m, 0], tiles[m, 3] = (ring[0], None), (ring[2], None)
        tiles[m, 1], tiles[m, 2] = (ring[1], 0), (ring[1], 1)

    sums_shape = (2 * router_weight.shape[1], tokens.shape[0])
    weights = (gate_other, up_other, gate_own, up_own)
    acc, squares, sums, down_own = early_of(gain, tiles, weights, down_proj, sums_shape)
    hidden, sums = late_of(gain, tiles, weights, acc, squares, sums)
    sums = along_z(sums, 0)

    places = [(0, 0), (0, ROWS), (1, 0), (1, ROWS)]
    far = down_of(True, [2 * ROWS] * 2, places, hidden, down_own, down_other)
    places = [(a, 0) for a in range(4)]
    places += [(4, 0), (5, 0), (8, 0), (8, ROWS)]
    places += [(9, 0), (10, 0), (6, 0), (7, 0)]
    shapes = [ROWS] * 8 + [2 * ROWS] + [ROWS] * 2
    rest = down_of(False, shapes, places, hidden, down_own, down_other)
    own, near, pair, singles = rest[:4], rest[4:8], rest[8], rest[9:]
    far_pairs = [hop(far[0], "z", "x-"), hop(far[1], "y", "x+")]
    far_in = [(far_pairs[n >> 1], (n & 1) * ROWS) for n in range(4)]
    pair_in = hop(pair, "y", "x-")
    singles_in = [hop(singles[n], "z", "x+") for n in range(2)]
    ways = [("y", "x-"), ("y", "x-"), ("z", "x+"), ("z", "x+")]
    near_in = [hop(added(near[n], far_in[n]), *ways[n]) for n in range(4)]
    parts = [
        (own[0], near_in[0], singles_in[0]),
        (own[1], near_in[1], singles_in[1]),
        (own[2], near_in[2], (pair_in, 0)),
        (own[3], near_in[3], (pair_in, ROWS)),
    ]
    terms = [
        *parts[0],
        hop(added(*parts[1]), "x-", "y"),
        hop(added(*parts[2]), "x+", "z"),
        hop(added(*parts[3]), "xx", "yz"),
    ]
    crossed = (CROSSED, width)
    stay, one, three, two, other = small(unpack_kernel, [block] * 3 + [crossed] * 2, *terms)
    other = across_y(other)
    one, three = along_z(one, 3), along_z(three, 1)
    stay = along_z(stay, 0)
    (far,) = small(join_kernel, [block], two, other)
    far = along_z(far, 2)
    keep, send = small(unshuffle_kernel, [(NEAR, width)] * 2, stay, one, three)
    came = across_y(send)
    slots = (2 * NEAR + BLOCK, tokens.shape[0])
    gates = small(partial(gates_kernel, width_all), [slots] * 2, ids, sums)
    return pl.pallas_call(
        combine_kernel,
        out_shape=jax.ShapeDtypeStruct(tokens.shape, BF16),
        in_specs=vmem(5),
        out_specs=vmem(1)[0],
        compiler_params=pltpu.CompilerParams(vmem_limit_bytes=4 << 20),
        name="combine",
    )(*gates, keep, came, far)


def solution(mesh):
    cut = Mesh(mesh.devices.reshape(SIZES), AXES)
    split = GRP + TP
    placed = (
        P(GRP, TP),
        P(),
        P(),
        P(GRP, None),
        P(None, split),
        P(None, split),
        P(split, None),
    )

    return jax.shard_map(per_device, mesh=cut, in_specs=placed, out_specs=P(GRP, TP), check_vma=False)
```
